32 devices in a mesh: blk: 8 (over z, x), lay: 4 (over y, core).
Axes of the slice: x: 2, y: 2, z: 4, core: 2. Of those that a mesh axis runs over, the one named last changes fastest.
Arguments:
- three_centre: bfloat16 [512, 512, 512], P('blk', 'lay'), may hold values from -224 to 224, as said below
- metric: bfloat16 [512, 64], P('blk'), may hold values from -2 to 6
- tile_pattern: int32 [512, 16, 16], P('blk'), may hold values from 0 to 1, as said below
- density: bfloat16 [512, 512], P('lay'), may hold values from -0.00048828125 to 0.00048828125
- dens_pattern: int32 [16, 16], replicated, may hold values 0 or 1
Outputs:
- exchange: float32 [512, 512], P('lay')
The draws below stay inside these ranges and needn't reach their ends.
Inputs may be any that keep to these rules, and one draw needn't show every extreme that they name: three_centre(P, mu, lambda) equals three_centre(P, lambda, mu). `tile_pattern`: symmetric in its last two dimensions; diagonal tiles are 1; the share of ones is drawn per group of 64 consecutive functions.
All inputs are finite; a program needn't handle non-finite values.
Results may differ from the reference program's by a relative error of at most 0.0043.
Values may be sent and summed in bfloat16 or wider, within the bound.
No kernel may reach another device: no remote copies, remote signals or barrier semaphores. Data moves between devices by JAX's collectives and lax.ppermute only.
A program may use at most 128 MiB of HBM per device.

```python
import math
import jax
import jax.numpy as jnp
from jax import lax

TILE = 32
NB = 16
AUXG = 64
NAUX = 512
NAO = 512


def draw_three_centre(key, part):
    groups = NAUX // AUXG
    scaling = 0.5 ** 0.5

    def draw_group(group_index):
        group_key = jax.random.fold_in(key, group_index)
        raw_draw = jnp.clip(jax.random.normal(group_key, (AUXG, NAO, NAO), jnp.float32), -5.0, 5.0)
        symmetric = (raw_draw + jnp.swapaxes(raw_draw, 1, 2)) * scaling
        return symmetric.astype(jnp.bfloat16)
    return lax.map(draw_group, jnp.arange(groups)).reshape(NAUX, NAO, NAO)


def draw_metric(key, part):
    local_index = jnp.arange(NAUX) % AUXG
    identity = (local_index[:, None] == jnp.arange(AUXG)[None, :]).astype(jnp.float32)
    noise_part = jnp.clip(jax.random.normal(key, (NAUX, AUXG), jnp.float32), -4.0, 4.0) * (0.6 / math.sqrt(AUXG))
    values = identity + noise_part
    return values.astype(jnp.bfloat16)


def draw_tile_pattern(key, part):
    groups = NAUX // AUXG
    levels = jax.random.randint(jax.random.fold_in(key, 11), (groups, 1, 1), 1, 5)
    levels = jnp.repeat(levels, AUXG, 0)
    raw_draw = jax.random.randint(jax.random.fold_in(key, 12), (NAUX, NB, NB), 0, 4)
    upper_part = jnp.triu(raw_draw)
    symmetric = upper_part + jnp.swapaxes(jnp.triu(raw_draw, 1), 1, 2)
    active = (symmetric < levels).astype(jnp.int32)
    identity = jnp.eye(NB, dtype=jnp.int32)
    return jnp.maximum(active, identity[None, :, :])


def set_ends(drawn, rng, smallest, largest):
    longest = drawn.shape.index(max(drawn.shape))
    spots = []
    for shift in (0, 1):
        where = [jax.random.randint(jax.random.fold_in(rng, axis), (), 0, length) for axis, length in enumerate(drawn.shape)]
        where[longest] = (where[longest] + shift) % drawn.shape[longest]
        spots.append(tuple(where))
    return drawn.at[spots[0]].set(smallest).at[spots[1]].set(largest)


def block_levels(own_key, shape, split, low, top_value):
    factor_of = 1.0
    for dim, parts in split:
        heights = jax.random.uniform(jax.random.fold_in(jax.random.fold_in(own_key, 6), dim), (parts,), jnp.float32, low / len(split), top_value / len(split))
        factor_of = factor_of * jnp.repeat(jnp.exp(heights), shape[dim] // parts).reshape((-1,) + (1,) * (len(shape) - 1 - dim))
    return factor_of


def normal_values(rng, extent, deviation, reach, cuts=(), kind=jnp.bfloat16):
    array = deviation * jax.random.normal(rng, extent, jnp.float32)
    if cuts:
        array = array * block_levels(rng, extent, cuts, -0.22, 0.18)
    return jnp.clip(array, -reach, reach).astype(kind)


def setup_inputs(seed: int = 0) -> dict:
    key_list = jax.random.split(jax.random.key(seed), 6)
    return {
        "three_centre": draw_three_centre(jax.random.fold_in(key_list[5], 71), 0),
        "metric": draw_metric(jax.random.fold_in(key_list[5], 71), 0),
        "tile_pattern": draw_tile_pattern(jax.random.fold_in(key_list[5], 71), 0),
        "density": normal_values(key_list[3], (NAO, NAO), (NAO * NAO * NAUX) ** -0.5, 0.00048828125, ((0, 4),)),
        "dens_pattern": set_ends((jax.random.randint(key_list[4], (NB, NB), 0, 4) < 3).astype(jnp.int32), jax.random.fold_in(key_list[4], 1), 0, 1),
    }


def reference(three_centre, metric, tile_pattern, density, dens_pattern):
    dens_mask = jnp.repeat(jnp.repeat(dens_pattern, TILE, 0), TILE, 1)
    kept = jnp.where(dens_mask > 0, density, jnp.zeros_like(density))
    groups = NAUX // AUXG
    integrals = three_centre.reshape(groups, AUXG, NAO, NAO)
    metrics = metric.reshape(groups, AUXG, AUXG)
    patterns = tile_pattern.reshape(groups, AUXG, NB, NB)

    def add_group(running, pieces):
        group_ints, group_metric, group_pattern = pieces
        tile_mask = jnp.repeat(jnp.repeat(group_pattern, TILE, 1), TILE, 2)
        masked = jnp.where(tile_mask > 0, group_ints, jnp.zeros_like(group_ints))
        coeffs = jnp.dot(group_metric, masked.reshape(AUXG, NAO * NAO), preferred_element_type=jnp.float32)
        coeffs = coeffs.astype(jnp.bfloat16).reshape(AUXG, NAO, NAO)
        inter = jnp.dot(coeffs.reshape(AUXG * NAO, NAO), kept, preferred_element_type=jnp.float32)
        inter = inter.astype(jnp.bfloat16).reshape(AUXG, NAO, NAO)
        group_part = jnp.einsum('pms,pns->mn', inter.astype(jnp.float32), coeffs.astype(jnp.float32))
        return running + group_part, None

    start_value = jnp.zeros((NAO, NAO), jnp.float32)
    exchange, unused = lax.scan(add_group, start_value, (integrals, metrics, patterns))
    return exchange
```

```python
import functools
import jax
import jax.numpy as jnp
from jax import lax
from jax.experimental import pallas as pl
from jax.experimental.pallas import tpu as pltpu
from jax.sharding import PartitionSpec as P

TILE = 32
SUB = 16
BF = jnp.bfloat16
F32 = jnp.float32


def density_adder(left_side, dens_pattern, segment):
    count = segment.shape[0]
    block_ids = jnp.arange(count, dtype=jnp.int32) // TILE
    row_pattern = jnp.take(dens_pattern, block_ids, axis=0)
    dens_mask = jnp.repeat(row_pattern, TILE, axis=1)
    kept = jnp.where(dens_mask > 0, segment, jnp.zeros_like(segment))
    return jnp.dot(left_side, kept, preferred_element_type=jnp.float32)


def per_device_any(three_centre, metric, tile_pattern, density, dens_pattern):
    group_size = three_centre.shape[0]
    row_count = three_centre.shape[1]
    ao_width = three_centre.shape[2]
    layers = lax.axis_size("lay")
    row_start = lax.axis_index("lay") * row_count
    row_blocks = (row_start + jnp.arange(row_count, dtype=jnp.int32)) // TILE
    pattern_rows = jnp.take(tile_pattern, row_blocks, axis=1)
    tile_mask = jnp.repeat(pattern_rows, TILE, axis=2)
    masked = jnp.where(tile_mask > 0, three_centre, jnp.zeros_like(three_centre))
    coeffs = jnp.einsum("pq,qmn->pmn", metric, masked, preferred_element_type=jnp.float32).astype(
        jnp.bfloat16
    )
    left_side = coeffs.reshape(group_size * row_count, ao_width)
    inter = density_adder(
        left_side, dens_pattern, lax.all_gather(density, "lay", axis=0, tiled=True)
    )
    column_count = ao_width // layers
    inter = inter.astype(jnp.bfloat16).reshape(group_size, row_count, layers, column_count)
    outgoing = jnp.transpose(inter, (2, 1, 0, 3)).reshape(
        layers, row_count, group_size * column_count
    )
    moved = lax.all_to_all(outgoing, "lay", split_axis=0, concat_axis=1, tiled=True)
    moved = moved.reshape(ao_width, group_size * column_count)
    partial_value = jnp.dot(
        moved, coeffs.reshape(group_size * row_count, ao_width), preferred_element_type=jnp.float32
    )
    row_sums = lax.psum_scatter(partial_value, "lay", scatter_dimension=0, tiled=True)
    return lax.psum(row_sums, "blk")


def dot(a, b):
    return jnp.dot(a, b, preferred_element_type=F32)


def dot_t(a, b):
    return lax.dot_general(a, b, (((1,), (1,)), ((), ())), preferred_element_type=F32)


def iota(shape, dim):
    return lax.broadcasted_iota(jnp.int32, shape, dim)


def spread_metric(l, metric_ref, spread_ref, orders):
    group = metric_ref.shape[0]
    part = group // 4
    rows, cols = part * SUB, group * SUB
    widen = (iota((rows, part), 0) // SUB == iota((rows, part), 1)).astype(BF)
    along = (iota((group, cols), 1) // SUB == iota((group, cols), 0)).astype(BF)
    same = iota((rows, cols), 0) % SUB == iota((rows, cols), 1) % SUB
    for n, p in enumerate(orders):
        start = pl.multiple_of((l ^ p) * part, part)
        tall = dot(widen, metric_ref[pl.ds(start, part), :]).astype(BF)
        full = dot(tall, along)
        spread_ref[n * rows : (n + 1) * rows, :] = jnp.where(same, full, 0.0).astype(BF)


def masked_columns(l, order, base, three_ref, pattern):
    group, sub, width = three_ref.shape
    block = pattern.shape[1] * TILE // 4
    tiles = pattern.shape[1]
    out = []
    for j in order:
        start = (l ^ j) * block
        here = (iota((tiles, block), 0) == (start // TILE) + iota((tiles, block), 1) // TILE).astype(BF)
        mask = dot(pattern, here).astype(BF)
        piece = three_ref[:, :, pl.ds(pl.multiple_of(start - base, block), block)]
        out.append((piece * mask[:, None, :]).reshape(group * sub, block))
    return jnp.concatenate(out, axis=1)


def near_kernel(l_ref, three_ref, metric_ref, pattern_ref, straight_ref, cross_ref, spread_ref):
    l = l_ref[0]

    @pl.when(pl.program_id(0) == 0)
    def _():
        spread_metric(l, metric_ref, spread_ref, (2, 3))

    part, sub, width = straight_ref.shape
    data = masked_columns(l, (0, 1), (l // 2) * width, three_ref, pattern_ref[0])
    got = dot(spread_ref[...], data).astype(BF)
    straight_ref[...] = got[: part * sub].reshape(part, sub, width)
    cross_ref[...] = got[part * sub :, : width // 2].reshape(part, sub, width // 2)


def rest_kernel(l_ref, three_ref, metric_ref, pattern_ref, keep_ref, send_ref, spread_ref):
    l = l_ref[0]

    @pl.when(pl.program_id(0) == 0)
    def _():
        spread_metric(l, metric_ref, spread_ref, (0, 2, 1, 3))

    both, part, sub, width = keep_ref.shape
    block = width // 4
    data = masked_columns(l, (0, 1, 2, 3), 0, three_ref, pattern_ref[0])
    half = 2 * part * sub
    keep_ref[...] = dot(spread_ref[:half], data).astype(BF).reshape(both, part, sub, width)
    got = dot(spread_ref[half:], data).astype(BF).reshape(both, part, sub, width)
    for j in range(4):
        send_ref[:, :, :, j * block : (j + 1) * block] = got[
            :, :, :, (j ^ 1) * block : ((j ^ 1) + 1) * block
        ]


def local_kernel(
    l_ref, mine_ref, peer_ref, d0_ref, d1_ref, d2_ref, d3_ref, dp_ref, own_ref, far_ref, left_ref, dens_ref, mask_ref
):
    l = l_ref[0]
    step = pl.program_id(0)
    width = mine_ref.shape[2]
    block = width // 4
    half = width // 2

    @pl.when(step == 0)
    def _():
        tiles = dp_ref.shape[0]
        pat = (dp_ref[...] > 0).astype(BF)
        tall = (iota((width, tiles), 0) // TILE == iota((width, tiles), 1)).astype(BF)
        wide = (iota((tiles, width), 1) // TILE == iota((tiles, width), 0)).astype(BF)
        mask_ref[...] = dot(dot(tall, pat).astype(BF), wide)
        for i, d_ref in enumerate((d0_ref, d1_ref, d2_ref, d3_ref)):
            r = pl.multiple_of((l ^ i) * block, block)
            for j in range(4):
                c = pl.multiple_of((l ^ j) * block, block)
                tile = d_ref[:, pl.ds(c, block)].astype(F32) * mask_ref[pl.ds(r, block), pl.ds(c, block)]
                dens_ref[i * block : (i + 1) * block, j * block : (j + 1) * block] = tile.astype(BF)
                dens_ref[j * block : (j + 1) * block, width + i * block : width + (i + 1) * block] = tile.T.astype(BF)
        own_ref[...] = jnp.zeros_like(own_ref)
        far_ref[...] = jnp.zeros_like(far_ref)

    count = mine_ref.shape[0]
    near = pl.num_programs(0) // 2

    @pl.when(step < near)
    def _():
        for n in range(count):
            rows = jnp.concatenate([mine_ref[n], peer_ref[n]], axis=0)
            both = dot(rows, dens_ref[...]).astype(BF)
            own_ref[...] += dot_t(both[:, :width], rows)
            far_ref[:half] += dot(both[:, :half], rows[:, half:])
            far_ref[half:] += dot(both[:, width : width + half], rows[:, half:])
            left_ref[n, :half] = both[:, half:width]
            left_ref[n, half:] = both[:, width + half :]

    @pl.when(step >= near)
    def _():
        for n in range(count):
            rows = jnp.concatenate([mine_ref[n], peer_ref[n]], axis=0)
            one = dot(rows, dens_ref[:, :width]).astype(BF)
            own_ref[...] += dot_t(one, rows)


def far_kernel(left_ref, straight_ref, cross_ref, begun_ref, keep_ref, send_ref, sum_ref):
    step = pl.program_id(0)
    count, block, half = straight_ref.shape

    @pl.when(step == 0)
    def _():
        sum_ref[...] = begun_ref[...]

    total = sum_ref[...]
    for n in range(count):
        top = straight_ref[n]
        low = jnp.concatenate([top[:, block:].T, cross_ref[n]], axis=1)
        total += dot(left_ref[n], jnp.concatenate([top, low], axis=0))
    sum_ref[...] = total

    @pl.when(step == pl.num_programs(0) - 1)
    def _():
        ab = sum_ref[:half]
        ba = sum_ref[half:].T
        keep_ref[:block] = ab[:block]
        keep_ref[block:] = ba[:block]
        send_ref[:block] = jnp.concatenate([ab[block:, block:], ab[block:, :block]], axis=1)
        send_ref[block:] = jnp.concatenate([ba[block:, block:], ba[block:, :block]], axis=1)


def call(kernel, grid, in_specs, out_specs, out_shape, scratch, flops, nbytes, name):
    return pl.pallas_call(
        kernel,
        grid_spec=pltpu.PrefetchScalarGridSpec(
            num_scalar_prefetch=1, grid=grid, in_specs=in_specs, out_specs=out_specs, scratch_shapes=scratch
        ),
        out_shape=out_shape,
        cost_estimate=pl.CostEstimate(flops=flops, bytes_accessed=nbytes, transcendentals=0),
        compiler_params=pltpu.CompilerParams(
            dimension_semantics=("arbitrary",), vmem_limit_bytes=40 * 1024 * 1024
        ),
        name=name,
    )


def swap(x, axis, bit):
    return lax.ppermute(x, axis, [(i, i ^ bit) for i in range(lax.axis_size(axis))])


def per_device_four(three, metric, tile_pattern, density, dens_pattern):
    group, block, width = three.shape
    part, half = group // 4, width // 2
    tiles = tile_pattern.shape[2]
    strips = block // SUB
    index = lax.axis_index("lay")
    l = jnp.reshape(index, (1,)).astype(jnp.int32)
    S = jax.ShapeDtypeStruct

    d1 = swap(density, "lay", 1)
    d2 = swap(density, "lay", 2)
    d3 = swap(d2, "lay", 1)

    pattern = lax.dynamic_slice(
        tile_pattern, (0, index * (block // TILE), 0), (group, block // TILE, tiles)
    )
    pattern = (jnp.transpose(pattern, (1, 0, 2)) > 0).astype(BF)
    per = TILE // SUB
    common = [
        pl.BlockSpec((group, group), lambda t, s: (0, 0)),
        pl.BlockSpec((1, group, tiles), lambda t, s: (t // per, 0, 0)),
    ]
    straight, cross = call(
        near_kernel,
        (strips,),
        [pl.BlockSpec((group, SUB, half), lambda t, s: (0, t, s[0] // 2))] + common,
        [
            pl.BlockSpec((part, SUB, half), lambda t, s: (0, t, 0)),
            pl.BlockSpec((part, SUB, block), lambda t, s: (0, t, 0)),
        ],
        [S((part, block, half), BF), S((part, block, block), BF)],
        [pltpu.VMEM((2 * part * SUB, group * SUB), BF)],
        2 * 2 * part * SUB * group * SUB * half * strips,
        group * block * half * 4,
        "near",
    )(l, three, metric, pattern)
    straight = swap(straight, "lay", 2)
    cross = swap(cross, "lay", 3)

    keep, send = call(
        rest_kernel,
        (strips,),
        [pl.BlockSpec((group, SUB, width), lambda t, s: (0, t, 0))] + common,
        [pl.BlockSpec((2, part, SUB, width), lambda t, s: (0, 0, t, 0))] * 2,
        [S((2, part, block, width), BF)] * 2,
        [pltpu.VMEM((group * SUB, group * SUB), BF)],
        2 * group * SUB * group * SUB * width * strips,
        group * block * width * 4,
        "rest",
    )(l, three, metric, pattern)
    peer = swap(send, "lay", 1)
    keep = keep.reshape(2 * part, block, width)
    peer = peer.reshape(2 * part, block, width)

    count = 2
    whole = lambda shape: pl.BlockSpec(shape, lambda t, s: (0,) * len(shape))
    own, far, left = call(
        local_kernel,
        (2 * part // count,),
        [pl.BlockSpec((count, block, width), lambda t, s: (t, 0, 0))] * 2
        + [whole((block, width))] * 4
        + [whole(dens_pattern.shape)],
        [
            whole((half, half)),
            whole((width, half)),
            pl.BlockSpec((count, width, half), lambda t, s: (jnp.minimum(t, part // count - 1), 0, 0)),
        ],
        [S((half, half), F32), S((width, half), F32), S((part, width, half), BF)],
        [pltpu.VMEM((width, 2 * width), BF), pltpu.VMEM((width, width), F32)],
        2 * part * (2 * half * width * width * 3 + 2 * half * width * half * 3),
        4 * part * block * width * 2 + part * width * half * 2,
        "local",
    )(l, keep, peer, density, d1, d2, d3, dens_pattern)

    count = 4
    kept, sent = call(
        lambda l_ref, *refs: far_kernel(*refs),
        (part // count,),
        [
            pl.BlockSpec((count, width, half), lambda t, s: (t, 0, 0)),
            pl.BlockSpec((count, block, half), lambda t, s: (t, 0, 0)),
            pl.BlockSpec((count, block, block), lambda t, s: (t, 0, 0)),
            whole((width, half)),
        ],
        [whole((half, half))] * 2,
        [S((half, half), F32)] * 2,
        [pltpu.VMEM((width, half), F32)],
        2 * part * width * half * half,
        part * width * half * 4,
        "far",
    )(l, left, straight, cross, far)

    own_sum = own[:block] + swap(
        jnp.concatenate([own[block:, block:], own[block:, :block]], axis=1), "lay", 1
    )
    far_sum = kept + swap(sent, "lay", 1)
    far_sum = far_sum[:block] + swap(far_sum[block:], "lay", 2)
    total = jnp.concatenate([own_sum, far_sum], axis=1)
    bit = 1
    while bit < lax.axis_size("blk"):
        total = total + swap(total, "blk", bit)
        bit *= 2
    odd, far_half = index % 2 == 1, index // 2 == 1
    pairs = total.reshape(block, 2, 2, block)
    pairs = jnp.where(odd, pairs[:, :, ::-1], pairs)
    pairs = jnp.where(far_half, pairs[:, ::-1], pairs)
    return pairs.reshape(block, width)


def solution(mesh):
    groups, layers = mesh.shape["blk"], mesh.shape["lay"]
    four = layers == 4 and groups & (groups - 1) == 0
    return jax.shard_map(
        per_device_four if four else per_device_any,
        mesh=mesh,
        in_specs=(P("blk", "lay", None), P("blk", None), P("blk", None, None), P("lay", None), P()),
        out_specs=P("lay", None),
        check_vma=False,
    )
```

```python
import functools
import jax
import jax.numpy as jnp
from jax import lax
from jax.experimental import pallas as pl
from jax.experimental.pallas import tpu as pltpu
from jax.sharding import PartitionSpec as P


TILE = 32
SUB = 16
BF = jnp.bfloat16
F32 = jnp.float32


def density_adder(left_side, dens_pattern, segment):
    count = segment.shape[0]
    block_ids = jnp.arange(count, dtype=jnp.int32) // TILE
    row_pattern = jnp.take(dens_pattern, block_ids, axis=0)
    dens_mask = jnp.repeat(row_pattern, TILE, axis=1)
    kept = jnp.where(dens_mask > 0, segment, jnp.zeros_like(segment))
    return jnp.dot(left_side, kept, preferred_element_type=jnp.float32)


def per_device_any(three_centre, metric, tile_pattern, density, dens_pattern):
    group_size = three_centre.shape[0]
    row_count = three_centre.shape[1]
    ao_width = three_centre.shape[2]
    layers = lax.axis_size("lay")
    row_start = lax.axis_index("lay") * row_count
    row_blocks = (row_start + jnp.arange(row_count, dtype=jnp.int32)) // TILE
    pattern_rows = jnp.take(tile_pattern, row_blocks, axis=1)
    tile_mask = jnp.repeat(pattern_rows, TILE, axis=2)
    masked = jnp.where(tile_mask > 0, three_centre, jnp.zeros_like(three_centre))
    coeffs = jnp.einsum("pq,qmn->pmn", metric, masked, preferred_element_type=jnp.float32).astype(
        jnp.bfloat16
    )
    left_side = coeffs.reshape(group_size * row_count, ao_width)
    inter = density_adder(
        left_side, dens_pattern, lax.all_gather(density, "lay", axis=0, tiled=True)
    )
    column_count = ao_width // layers
    inter = inter.astype(jnp.bfloat16).reshape(group_size, row_count, layers, column_count)
    outgoing = jnp.transpose(inter, (2, 1, 0, 3)).reshape(
        layers, row_count, group_size * column_count
    )
    moved = lax.all_to_all(outgoing, "lay", split_axis=0, concat_axis=1, tiled=True)
    moved = moved.reshape(ao_width, group_size * column_count)
    partial_value = jnp.dot(
        moved, coeffs.reshape(group_size * row_count, ao_width), preferred_element_type=jnp.float32
    )
    row_sums = lax.psum_scatter(partial_value, "lay", scatter_dimension=0, tiled=True)
    return lax.psum(row_sums, "blk")


def dot(a, b):
    return jnp.dot(a, b, preferred_element_type=F32)


def dot_t(a, b):
    return lax.dot_general(a, b, (((1,), (1,)), ((), ())), preferred_element_type=F32)


def iota(shape, dim):
    return lax.broadcasted_iota(jnp.int32, shape, dim)


def spread_metric(l, metric_ref, spread_ref, orders):
    group = metric_ref.shape[0]
    part = group // 4
    rows, cols = part * SUB, group * SUB
    widen = (iota((rows, part), 0) // SUB == iota((rows, part), 1)).astype(BF)
    along = (iota((group, cols), 1) // SUB == iota((group, cols), 0)).astype(BF)
    same = iota((rows, cols), 0) % SUB == iota((rows, cols), 1) % SUB
    for n, p in enumerate(orders):
        start = pl.multiple_of((l ^ p) * part, part)
        tall = dot(widen, metric_ref[pl.ds(start, part), :]).astype(BF)
        full = dot(tall, along)
        spread_ref[n * rows : (n + 1) * rows, :] = jnp.where(same, full, 0.0).astype(BF)


def masked_columns(l, order, base, three_ref, pattern_ref):
    group, sub, _ = three_ref.shape
    tiles = pattern_ref.shape[1]
    block = tiles * TILE // 4
    pattern = (pattern_ref[0] > 0).astype(BF)
    out = []
    for j in order:
        start = (l ^ j) * block
        here = (iota((tiles, block), 0) == (start // TILE) + iota((tiles, block), 1) // TILE).astype(BF)
        mask = lax.dot_general(pattern, here, (((0,), (0,)), ((), ())), preferred_element_type=F32)
        mask = jnp.broadcast_to(mask[:, None, :], (group, sub, block)).astype(BF)
        piece = three_ref[:, :, pl.ds(pl.multiple_of(start - base, block), block)]
        out.append((piece * mask).reshape(group * sub, block))
    return jnp.concatenate(out, axis=1)


def near_kernel(l_ref, three_ref, metric_ref, pattern_ref, straight_ref, cross_ref, core_ref, spread_ref):
    l = l_ref[0]

    @pl.when(pl.program_id(0) == 0)
    def _():
        spread_metric(l, metric_ref, spread_ref, (2, 3))

    part, sub, width = straight_ref.shape
    block = width // 2
    data = masked_columns(l, (0, 1), (l // 2) * width, three_ref, pattern_ref)
    got = dot(spread_ref[...], data).astype(BF)
    straight_ref[...] = got[: part * sub].reshape(part, sub, width)
    low = got[part * sub :].reshape(part, sub, width)
    cross_ref[...] = low[:, :, :block]
    core_ref[:, :, :block] = low[:, :, block:]
    core_ref[:, :, block:] = low[:, :, :block]


def swapped(x, block):
    parts = []
    for j in range(x.shape[-1] // block):
        k = j ^ 1
        parts.append(x[..., k * block : (k + 1) * block])
    return jnp.concatenate(parts, axis=-1)


def rest_kernel(l_ref, three_ref, metric_ref, pattern_ref, keep_ref, send_ref, spread_ref, *, cut, orders):
    l = l_ref[0]

    @pl.when(pl.program_id(0) == 0)
    def _():
        spread_metric(l, metric_ref, spread_ref, orders)

    part, sub, width = keep_ref.shape
    block = width // len(cut)
    base = (l ^ cut[0]) // 2 * width if len(cut) == 2 else 0
    data = masked_columns(l, cut, base, three_ref, pattern_ref)
    got = dot(spread_ref[...], data).astype(BF)
    keep_ref[...] = got[: part * sub].reshape(part, sub, width)
    send_ref[...] = swapped(got[part * sub :].reshape(part, sub, width), block)


def settle_kernel(l_ref, d0_ref, d1_ref, d2_ref, d3_ref, dp_ref, dens_ref, mask_ref):
    l = l_ref[0]
    block, width = d0_ref.shape
    tiles = dp_ref.shape[0]
    pat = (dp_ref[...] > 0).astype(BF)
    tall = (iota((width, tiles), 0) // TILE == iota((width, tiles), 1)).astype(BF)
    wide = (iota((tiles, width), 1) // TILE == iota((tiles, width), 0)).astype(BF)
    mask_ref[...] = dot(dot(tall, pat).astype(BF), wide)
    for i, d_ref in enumerate((d0_ref, d1_ref, d2_ref, d3_ref)):
        r = pl.multiple_of((l ^ i) * block, block)
        for j in range(4):
            c = pl.multiple_of((l ^ j) * block, block)
            tile = d_ref[:, pl.ds(c, block)].astype(F32) * mask_ref[pl.ds(r, block), pl.ds(c, block)]
            dens_ref[i * block : (i + 1) * block, j * block : (j + 1) * block] = tile.astype(BF)
            dens_ref[j * block : (j + 1) * block, width + i * block : width + (i + 1) * block] = tile.T.astype(BF)


def own_kernel(a_ref, pa_ref, b0_ref, b1_ref, pb0_ref, pb1_ref, dens_ref, inter_ref, keep_ref, send_ref, sum_ref):
    step = pl.program_id(0)
    count, block, _ = a_ref.shape
    dens = dens_ref[...]

    @pl.when(step == 0)
    def _():
        sum_ref[...] = jnp.zeros_like(sum_ref)

    total = sum_ref[...]
    for n in range(count):
        rows = jnp.concatenate([a_ref[n], pa_ref[n]], axis=0)
        inter = dot(rows, dens).astype(BF)
        inter_ref[n] = inter
        total += dot_t(inter, rows)
        top = jnp.concatenate([b0_ref[n], b1_ref[n]], axis=1)
        low = jnp.concatenate([pb0_ref[n], pb1_ref[n]], axis=1)
        rows = jnp.concatenate([top, low], axis=0)
        total += dot_t(dot(rows, dens).astype(BF), rows)
    sum_ref[...] = total

    @pl.when(step == pl.num_programs(0) - 1)
    def _():
        keep_ref[...] = total[:block]
        send_ref[...] = swapped(total[block:], block)


def local_kernel(a_ref, pa_ref, inter_ref, dens_ref, left_ref, far_ref):
    step = pl.program_id(0)
    count, _, width = a_ref.shape
    half = width // 2

    @pl.when(step == 0)
    def _():
        far_ref[...] = jnp.zeros_like(far_ref)

    dens = dens_ref[...]
    for n in range(count):
        rows = jnp.concatenate([a_ref[n], pa_ref[n]], axis=0)
        turned = dot(rows, dens).astype(BF)
        side = rows[:, half:]
        far_ref[:half] += dot(inter_ref[n, :, :half], side)
        far_ref[half:] += dot(turned[:, :half], side)
        left_ref[n, :half] = inter_ref[n, :, half:]
        left_ref[n, half:] = turned[:, half:]


def far_kernel(left_ref, straight_ref, cross_ref, begun_ref, keep_ref, send_ref, sum_ref):
    step = pl.program_id(0)
    count, block, half = straight_ref.shape

    @pl.when(step == 0)
    def _():
        sum_ref[...] = begun_ref[...]

    total = sum_ref[...]
    for n in range(count):
        top = straight_ref[n]
        low = jnp.concatenate([top[:, block:].T, cross_ref[n]], axis=1)
        total += dot(left_ref[n], jnp.concatenate([top, low], axis=0))
    sum_ref[...] = total

    @pl.when(step == pl.num_programs(0) - 1)
    def _():
        ab = total[:half]
        ba = total[half:].T
        keep_ref[:block] = ab[:block]
        keep_ref[block:] = ba[:block]
        send_ref[:block] = swapped(ab[block:], block)
        send_ref[block:] = swapped(ba[block:], block)


def place_kernel(l_ref, own_ref, own_got_ref, far_ref, far_got_ref, out_ref):
    l = l_ref[0]
    block = out_ref.shape[0]
    for j, (a_ref, b_ref) in enumerate(((own_ref, own_got_ref),) * 2 + ((far_ref, far_got_ref),) * 2):
        at = j % 2 * block
        total = a_ref[:, at : at + block] + b_ref[:, at : at + block].astype(F32)
        out_ref[:, pl.ds(pl.multiple_of((l ^ j) * block, block), block)] = total


def call(kernel, grid, in_specs, out_specs, out_shape, scratch, flops, nbytes, vmem=20):
    return pl.pallas_call(
        kernel,
        grid_spec=pltpu.PrefetchScalarGridSpec(
            num_scalar_prefetch=1, grid=grid, in_specs=in_specs, out_specs=out_specs, scratch_shapes=scratch
        ),
        out_shape=out_shape,
        cost_estimate=pl.CostEstimate(flops=flops, bytes_accessed=nbytes, transcendentals=0),
        compiler_params=pltpu.CompilerParams(
            dimension_semantics=("arbitrary",), vmem_limit_bytes=vmem * 1024 * 1024
        ),
    )


def no_index(kernel):
    return lambda l_ref, *refs: kernel(*refs)


def swap(x, axis, bit):
    return lax.ppermute(x, axis, [(i, i ^ bit) for i in range(lax.axis_size(axis))])


def rounded(x):
    return lax.reduce_precision(x, 8, 7)


def bits_of(groups):
    return [1 << n for n in range(groups.bit_length() - 1)]


def per_device_four(three, metric, tile_pattern, density, dens_pattern):
    return exchange_four(three, metric, tile_pattern, density, dens_pattern)


def exchange_four(three, metric, tile_pattern, density, dens_pattern):
    group, block, width = three.shape
    part, half = group // 4, width // 2
    tiles = tile_pattern.shape[2]
    strips = block // SUB
    index = lax.axis_index("lay")
    l = jnp.reshape(index, (1,)).astype(jnp.int32)
    S = jax.ShapeDtypeStruct
    whole = lambda shape: pl.BlockSpec(shape, lambda t, s: (0,) * len(shape))

    d2 = swap(density, "lay", 2)
    d1 = swap(density, "lay", 1)
    d3 = swap(d2, "lay", 1)

    pattern = jnp.transpose(tile_pattern, (1, 2, 0))
    per, here = TILE // SUB, block // TILE
    common = [
        pl.BlockSpec((group, group), lambda t, s: (0, 0)),
        pl.BlockSpec((1, tiles, group), lambda t, s: (s[0] * here + t // per, 0, 0)),
    ]
    strip = lambda n: pl.BlockSpec((part, SUB, n), lambda t, s: (0, t, 0))
    straight, cross, send3 = call(
        near_kernel,
        (strips,),
        [pl.BlockSpec((group, SUB, half), lambda t, s: (0, t, s[0] // 2))] + common,
        [strip(half), strip(block), strip(half)],
        [S((part, block, half), BF), S((part, block, block), BF), S((part, block, half), BF)],
        [pltpu.VMEM((2 * part * SUB, group * SUB), BF)],
        2 * 2 * part * SUB * group * SUB * half * strips,
        group * block * half * 4,
        vmem=NEAR_VMEM,
    )(l, three, metric, pattern)
    far_straight = swap(straight, "lay", 2)
    far_cross = swap(cross, "lay", 3)
    got3 = swap(send3, "lay", 1)

    def rest(cut, orders, columns):
        n = len(cut) * block
        return call(
            functools.partial(rest_kernel, cut=cut, orders=orders),
            (strips,),
            [pl.BlockSpec((group, SUB, n), columns)] + common,
            [strip(n)] * 2,
            [S((part, block, n), BF)] * 2,
            [pltpu.VMEM((2 * part * SUB, group * SUB), BF)],
            2 * 2 * part * SUB * group * SUB * n * strips,
            group * block * n * 4,
            vmem=NEAR_VMEM,
        )(l, three, metric, pattern)

    keep0, send1 = rest((0, 1, 2, 3), (0, 1), lambda t, s: (0, t, 0))
    got1 = swap(send1, "lay", 1)
    keep2, send4 = rest((2, 3), (2, 3), lambda t, s: (0, t, 1 - s[0] // 2))
    got4 = swap(send4, "lay", 1)

    dens = call(
        settle_kernel,
        (1,),
        [whole((block, width))] * 4 + [whole(dens_pattern.shape)],
        whole((width, 2 * width)),
        S((width, 2 * width), BF),
        [pltpu.VMEM((width, width), F32)],
        4 * width * width * tiles,
        4 * width * width * 2,
    )(l, density, d1, d2, d3, dens_pattern)

    count = 2
    many = lambda a, b: pl.BlockSpec((count, a, b), lambda t, s: (t, 0, 0))
    inter, own_keep, own_send = call(
        no_index(own_kernel),
        (part // count,),
        [many(block, width)] * 2 + [many(block, half)] * 4 + [pl.BlockSpec((width, width), lambda t, s: (0, 0))],
        [many(half, width), whole((block, half)), whole((block, half))],
        [S((part, half, width), BF), S((block, half), F32), S((block, half), F32)],
        [pltpu.VMEM((half, half), F32)],
        2 * part * 2 * half * width * (width + half),
        2 * part * half * width * 2,
    )(l, keep0, got1, straight, keep2, got3, got4, dens)
    own = own_keep + swap(own_send, "lay", 1)

    left, far = call(
        no_index(local_kernel),
        (part // count,),
        [many(block, width)] * 2
        + [many(half, width), pl.BlockSpec((width, width), lambda t, s: (0, 1))],
        [many(width, half), whole((width, half))],
        [S((part, width, half), BF), S((width, half), F32)],
        [],
        part * 2 * half * (width * width + 2 * half * half),
        part * half * width * 8,
    )(l, keep0, got1, inter, dens)

    count = 4
    kept, sent = call(
        no_index(far_kernel),
        (part // count,),
        [many(width, half), many(block, half), many(block, block), whole((width, half))],
        [whole((half, half))] * 2,
        [S((half, half), F32)] * 2,
        [pltpu.VMEM((width, half), F32)],
        2 * part * width * half * half,
        part * width * half * 4,
    )(l, left, far_straight, far_cross, far)
    far = kept + swap(sent, "lay", 1)
    far = far[:block] + swap(far[block:].astype(BF), "lay", 2).astype(F32)

    def over_groups(x):
        steps = bits_of(lax.axis_size("blk"))
        for n, bit in enumerate(steps):
            x = rounded(x)
            got = swap(x.astype(BF), "blk", bit if n < 2 else bit | steps[n - 1])
            if n == len(steps) - 1:
                return x, got
            x = x + got.astype(F32)
        return x, jnp.zeros(x.shape, BF)

    own, own_got = over_groups(own)
    far, far_got = over_groups(far)
    return call(
        place_kernel,
        (1,),
        [whole((block, half))] * 4,
        whole((block, width)),
        S((block, width), F32),
        [],
        block * width,
        block * width * 10,
    )(l, own, own_got, far, far_got)


NEAR_VMEM = 57


def solution(mesh):
    groups, layers = mesh.shape["blk"], mesh.shape["lay"]
    four = layers == 4 and groups & (groups - 1) == 0
    return jax.shard_map(
        per_device_four if four else per_device_any,
        mesh=mesh,
        in_specs=(P("blk", "lay", None), P("blk", None), P("blk", None, None), P("lay", None), P()),
        out_specs=P("lay", None),
        check_vma=False,
    )
```

```python
import jax
import jax.numpy as jnp
from jax import lax
from jax.experimental import pallas as pl
from jax.experimental.pallas import tpu as pltpu
from jax.sharding import PartitionSpec as P


TILE = 32
SUB = 16
BF = jnp.bfloat16
F32 = jnp.float32


def density_adder(left_side, dens_pattern, segment):
    count = segment.shape[0]
    block_ids = jnp.arange(count, dtype=jnp.int32) // TILE
    row_pattern = jnp.take(dens_pattern, block_ids, axis=0)
    dens_mask = jnp.repeat(row_pattern, TILE, axis=1)
    kept = jnp.where(dens_mask > 0, segment, jnp.zeros_like(segment))
    return jnp.dot(left_side, kept, preferred_element_type=jnp.float32)


def per_device_any(three_centre, metric, tile_pattern, density, dens_pattern):
    group_size = three_centre.shape[0]
    row_count = three_centre.shape[1]
    ao_width = three_centre.shape[2]
    layers = lax.axis_size("lay")
    row_start = lax.axis_index("lay") * row_count
    row_blocks = (row_start + jnp.arange(row_count, dtype=jnp.int32)) // TILE
    pattern_rows = jnp.take(tile_pattern, row_blocks, axis=1)
    tile_mask = jnp.repeat(pattern_rows, TILE, axis=2)
    masked = jnp.where(tile_mask > 0, three_centre, jnp.zeros_like(three_centre))
    coeffs = jnp.einsum("pq,qmn->pmn", metric, masked, preferred_element_type=jnp.float32).astype(
        jnp.bfloat16
    )
    left_side = coeffs.reshape(group_size * row_count, ao_width)
    inter = density_adder(
        left_side, dens_pattern, lax.all_gather(density, "lay", axis=0, tiled=True)
    )
    column_count = ao_width // layers
    inter = inter.astype(jnp.bfloat16).reshape(group_size, row_count, layers, column_count)
    outgoing = jnp.transpose(inter, (2, 1, 0, 3)).reshape(
        layers, row_count, group_size * column_count
    )
    moved = lax.all_to_all(outgoing, "lay", split_axis=0, concat_axis=1, tiled=True)
    moved = moved.reshape(ao_width, group_size * column_count)
    partial_value = jnp.dot(
        moved, coeffs.reshape(group_size * row_count, ao_width), preferred_element_type=jnp.float32
    )
    row_sums = lax.psum_scatter(partial_value, "lay", scatter_dimension=0, tiled=True)
    return lax.psum(row_sums, "blk")


def dot(a, b):
    return jnp.dot(a, b, preferred_element_type=F32)


def dot_t(a, b):
    return lax.dot_general(a, b, (((1,), (1,)), ((), ())), preferred_element_type=F32)


def iota(shape, dim):
    return lax.broadcasted_iota(jnp.int32, shape, dim)


def spread_metric(l, metric_ref, spread_ref, orders):
    group = metric_ref.shape[0]
    part = group // 4
    rows, cols = part * SUB, group * SUB
    widen = (iota((rows, part), 0) // SUB == iota((rows, part), 1)).astype(BF)
    along = (iota((group, cols), 1) // SUB == iota((group, cols), 0)).astype(BF)
    same = iota((rows, cols), 0) % SUB == iota((rows, cols), 1) % SUB
    for n, p in enumerate(orders):
        start = pl.multiple_of((l ^ p) * part, part)
        tall = dot(widen, metric_ref[pl.ds(start, part), :]).astype(BF)
        full = dot(tall, along)
        spread_ref[n * rows : (n + 1) * rows, :] = jnp.where(same, full, 0.0).astype(BF)


def masked_columns(l, order, base, three_ref, pattern_ref, first):
    group = three_ref.shape[0]
    tiles = pattern_ref.shape[1]
    block = tiles * TILE // 4
    pattern = (pattern_ref[first // TILE] > 0).astype(BF)
    out = [[] for _ in range(TILE // SUB)]
    for j in order:
        start = (l ^ j) * block
        here = (iota((tiles, block), 0) == (start // TILE) + iota((tiles, block), 1) // TILE).astype(BF)
        mask = lax.dot_general(pattern, here, (((0,), (0,)), ((), ())), preferred_element_type=F32)
        mask = jnp.broadcast_to(mask[:, None, :], (group, SUB, block)).astype(BF)
        for n, pieces in enumerate(out):
            at = first + n * SUB
            piece = three_ref[:, at : at + SUB, pl.ds(pl.multiple_of(start - base, block), block)]
            pieces.append((piece * mask).reshape(group * SUB, block))
    return [jnp.concatenate(pieces, axis=1) for pieces in out]


def near_kernel(l_ref, three_ref, metric_ref, pattern_ref, straight_ref, cross_ref, core_ref, spread_ref):
    l = l_ref[0]

    @pl.when(pl.program_id(0) == 0)
    def _():
        spread_metric(l, metric_ref, spread_ref, (2, 3))

    part, rows, width = straight_ref.shape
    block = width // 2
    for first in range(0, rows, TILE):
        strips = masked_columns(l, (0, 1), (l // 2) * width, three_ref, pattern_ref, first)
        for n, data in enumerate(strips):
            at = slice(first + n * SUB, first + (n + 1) * SUB)
            got = dot(spread_ref[...], data).astype(BF)
            straight_ref[:, at] = got[: part * SUB].reshape(part, SUB, width)
            low = got[part * SUB :].reshape(part, SUB, width)
            cross_ref[:, at] = low[:, :, :block]
            core_ref[:, at] = swapped(low, block)


def swapped(x, block):
    parts = []
    for j in range(x.shape[-1] // block):
        k = j ^ 1
        parts.append(x[..., k * block : (k + 1) * block])
    return jnp.concatenate(parts, axis=-1)


def rest_kernel(
    l_ref, three_ref, metric_ref, pattern_ref, keep_ref, send_ref, keep_far_ref, send_far_ref, spread_ref
):
    l = l_ref[0]

    @pl.when(pl.program_id(0) == 0)
    def _():
        spread_metric(l, metric_ref, spread_ref, (0, 1, 2, 3))

    part, rows, width = keep_ref.shape
    half, block = width // 2, width // 4
    one = part * SUB
    for first in range(0, rows, TILE):
        strips = masked_columns(l, (0, 1, 2, 3), 0, three_ref, pattern_ref, first)
        for n, data in enumerate(strips):
            at = slice(first + n * SUB, first + (n + 1) * SUB)
            got = dot(spread_ref[: 2 * one], data).astype(BF)
            keep_ref[:, at] = got[:one].reshape(part, SUB, width)
            send_ref[:, at] = swapped(got[one:].reshape(part, SUB, width), block)
            got = dot(spread_ref[2 * one :], data[:, half:]).astype(BF)
            keep_far_ref[:, at] = got[:one].reshape(part, SUB, half)
            send_far_ref[:, at] = swapped(got[one:].reshape(part, SUB, half), block)


def settle_kernel(l_ref, d0_ref, d1_ref, d2_ref, d3_ref, dp_ref, dens_ref, mask_ref):
    l = l_ref[0]
    block, width = d0_ref.shape
    tiles = dp_ref.shape[0]
    pat = (dp_ref[...] > 0).astype(BF)
    tall = (iota((width, tiles), 0) // TILE == iota((width, tiles), 1)).astype(BF)
    wide = (iota((tiles, width), 1) // TILE == iota((tiles, width), 0)).astype(BF)
    mask_ref[...] = dot(dot(tall, pat).astype(BF), wide)
    for i, d_ref in enumerate((d0_ref, d1_ref, d2_ref, d3_ref)):
        r = pl.multiple_of((l ^ i) * block, block)
        for j in range(4):
            c = pl.multiple_of((l ^ j) * block, block)
            tile = d_ref[:, pl.ds(c, block)].astype(F32) * mask_ref[pl.ds(r, block), pl.ds(c, block)]
            dens_ref[i * block : (i + 1) * block, j * block : (j + 1) * block] = tile.astype(BF)
            dens_ref[j * block : (j + 1) * block, width + i * block : width + (i + 1) * block] = tile.T.astype(BF)


def own_kernel(a_ref, pa_ref, b0_ref, b1_ref, pb0_ref, pb1_ref, dens_ref, inter_ref, keep_ref, send_ref, sum_ref):
    step = pl.program_id(0)
    count, block, _ = a_ref.shape
    dens = dens_ref[...]

    @pl.when(step == 0)
    def _():
        sum_ref[...] = jnp.zeros_like(sum_ref)

    total = sum_ref[...]
    for n in range(count):
        rows = jnp.concatenate([a_ref[n], pa_ref[n]], axis=0)
        inter = dot(rows, dens).astype(BF)
        inter_ref[n] = inter
        total += dot_t(inter, rows)
        top = jnp.concatenate([b0_ref[n], b1_ref[n]], axis=1)
        low = jnp.concatenate([pb0_ref[n], pb1_ref[n]], axis=1)
        rows = jnp.concatenate([top, low], axis=0)
        total += dot_t(dot(rows, dens).astype(BF), rows)
    sum_ref[...] = total

    @pl.when(step == pl.num_programs(0) - 1)
    def _():
        keep_ref[...] = total[:block]
        send_ref[...] = swapped(total[block:], block)


def local_kernel(a_ref, pa_ref, inter_ref, dens_ref, left_ref, far_ref):
    step = pl.program_id(0)
    count, _, width = a_ref.shape
    half = width // 2

    @pl.when(step == 0)
    def _():
        far_ref[...] = jnp.zeros_like(far_ref)

    dens = dens_ref[...]
    for n in range(count):
        rows = jnp.concatenate([a_ref[n], pa_ref[n]], axis=0)
        turned = dot(rows, dens).astype(BF)
        side = rows[:, half:]
        far_ref[:half] += dot(inter_ref[n, :, :half], side)
        far_ref[half:] += dot(turned[:, :half], side)
        left_ref[n, :half] = inter_ref[n, :, half:]
        left_ref[n, half:] = turned[:, half:]


def far_kernel(left_ref, straight_ref, cross_ref, begun_ref, keep_ref, send_ref, sum_ref):
    step = pl.program_id(0)
    count, block, half = straight_ref.shape

    @pl.when(step == 0)
    def _():
        sum_ref[...] = begun_ref[...]

    total = sum_ref[...]
    for n in range(count):
        top = straight_ref[n]
        low = jnp.concatenate([top[:, block:].T, cross_ref[n]], axis=1)
        total += dot(left_ref[n], jnp.concatenate([top, low], axis=0))
    sum_ref[...] = total

    @pl.when(step == pl.num_programs(0) - 1)
    def _():
        ab = total[:half]
        ba = total[half:].T
        keep_ref[:block] = ab[:block]
        keep_ref[block:] = ba[:block]
        send_ref[:block] = swapped(ab[block:], block)
        send_ref[block:] = swapped(ba[block:], block)


def place_kernel(l_ref, mine_ref, got_ref, out_ref):
    l = l_ref[0]
    block, _ = out_ref.shape
    for j in range(4):
        at = slice(j * block, (j + 1) * block)
        total = mine_ref[:, at] + got_ref[:, at].astype(F32)
        out_ref[:, pl.ds(pl.multiple_of((l ^ j) * block, block), block)] = total


def call(kernel, grid, in_specs, out_specs, out_shape, scratch, flops, nbytes, vmem=20):
    return pl.pallas_call(
        kernel,
        grid_spec=pltpu.PrefetchScalarGridSpec(
            num_scalar_prefetch=1, grid=grid, in_specs=in_specs, out_specs=out_specs, scratch_shapes=scratch
        ),
        out_shape=out_shape,
        cost_estimate=pl.CostEstimate(flops=flops, bytes_accessed=nbytes, transcendentals=0),
        compiler_params=pltpu.CompilerParams(
            dimension_semantics=("arbitrary",), vmem_limit_bytes=vmem * 1024 * 1024
        ),
    )


def no_index(kernel):
    return lambda l_ref, *refs: kernel(*refs)


def swap(x, axis, bit):
    return lax.ppermute(x, axis, [(i, i ^ bit) for i in range(lax.axis_size(axis))])


def rounded(x):
    return lax.reduce_precision(x, 8, 7)


def bits_of(groups):
    return [1 << n for n in range(groups.bit_length() - 1)]


def per_device_four(three, metric, tile_pattern, density, dens_pattern):
    return exchange_four(three, metric, tile_pattern, density, dens_pattern)


def exchange_four(three, metric, tile_pattern, density, dens_pattern):
    group, block, width = three.shape
    part, half = group // 4, width // 2
    tiles = tile_pattern.shape[2]
    index = lax.axis_index("lay")
    l = jnp.reshape(index, (1,)).astype(jnp.int32)
    S = jax.ShapeDtypeStruct
    whole = lambda shape: pl.BlockSpec(shape, lambda t, s: (0,) * len(shape))

    d2 = swap(density, "lay", 2)
    d1 = swap(density, "lay", 1)
    d3 = swap(d2, "lay", 1)

    pattern = jnp.transpose(tile_pattern, (1, 2, 0))
    metric_spec = pl.BlockSpec((group, group), lambda t, s: (0, 0))

    def pattern_spec(rows):
        return pl.BlockSpec((rows // TILE, tiles, group), lambda t, s: (s[0] * (block // rows) + t, 0, 0))

    rows = 2 * TILE
    strip = lambda n: pl.BlockSpec((part, 2 * TILE, n), lambda t, s: (0, t, 0))
    straight, cross, send3 = call(
        near_kernel,
        (block // rows,),
        [pl.BlockSpec((group, rows, half), lambda t, s: (0, t, s[0] // 2)), metric_spec, pattern_spec(rows)],
        [strip(half), strip(block), strip(half)],
        [S((part, block, half), BF), S((part, block, block), BF), S((part, block, half), BF)],
        [pltpu.VMEM((2 * part * SUB, group * SUB), BF)],
        4 * part * SUB * group * half * block,
        group * block * half * 4,
        vmem=57,
    )(l, three, metric, pattern)
    far_straight = swap(straight, "lay", 2)
    far_cross = swap(cross, "lay", 3)
    got3 = swap(send3, "lay", 1)

    tile = lambda n: pl.BlockSpec((part, TILE, n), lambda t, s: (0, t, 0))
    keep0, send1, keep2, send4 = call(
        rest_kernel,
        (block // TILE,),
        [pl.BlockSpec((group, TILE, width), lambda t, s: (0, t, 0)), metric_spec, pattern_spec(TILE)],
        [tile(width)] * 2 + [tile(half)] * 2,
        [S((part, block, width), BF)] * 2 + [S((part, block, half), BF)] * 2,
        [pltpu.VMEM((group * SUB, group * SUB), BF)],
        6 * part * SUB * group * width * block,
        group * block * width * 4,
        vmem=57,
    )(l, three, metric, pattern)
    got1 = swap(send1, "lay", 1)
    got4 = swap(send4, "lay", 1)

    dens = call(
        settle_kernel,
        (1,),
        [whole((block, width))] * 4 + [whole(dens_pattern.shape)],
        whole((width, 2 * width)),
        S((width, 2 * width), BF),
        [pltpu.VMEM((width, width), F32)],
        4 * width * width * tiles,
        4 * width * width * 2,
    )(l, density, d1, d2, d3, dens_pattern)

    count = 2
    many = lambda a, b: pl.BlockSpec((count, a, b), lambda t, s: (t, 0, 0))
    inter, own_keep, own_send = call(
        no_index(own_kernel),
        (part // count,),
        [many(block, width)] * 2 + [many(block, half)] * 4 + [pl.BlockSpec((width, width), lambda t, s: (0, 0))],
        [many(half, width), whole((block, half)), whole((block, half))],
        [S((part, half, width), BF), S((block, half), F32), S((block, half), F32)],
        [pltpu.VMEM((half, half), F32)],
        2 * part * 2 * half * width * (width + half),
        2 * part * half * width * 2,
        vmem=57,
    )(l, keep0, got1, straight, keep2, got3, got4, dens)
    own = own_keep + swap(own_send, "lay", 1)

    count = 4
    left, far = call(
        no_index(local_kernel),
        (part // count,),
        [many(block, width)] * 2
        + [many(half, width), pl.BlockSpec((width, width), lambda t, s: (0, 1))],
        [many(width, half), whole((width, half))],
        [S((part, width, half), BF), S((width, half), F32)],
        [],
        part * 2 * half * (width * width + 2 * half * half),
        part * half * width * 8,
        vmem=57,
    )(l, keep0, got1, inter, dens)

    count = 4
    kept, sent = call(
        no_index(far_kernel),
        (part // count,),
        [many(width, half), many(block, half), many(block, block), whole((width, half))],
        [whole((half, half))] * 2,
        [S((half, half), F32)] * 2,
        [pltpu.VMEM((width, half), F32)],
        2 * part * width * half * half,
        part * width * half * 4,
        vmem=57,
    )(l, left, far_straight, far_cross, far)
    far = kept + swap(sent, "lay", 1)
    far = far[:block] + swap(far[block:].astype(BF), "lay", 2).astype(F32)

    steps = bits_of(lax.axis_size("blk"))
    for bit in steps[:-1]:
        own = own + swap(own, "blk", bit)
        far = rounded(far)
        far = far + swap(far.astype(BF), "blk", bit).astype(F32)
    total = rounded(jnp.concatenate([own, far], axis=1))
    got = jnp.zeros(total.shape, BF)
    if steps:
        got = swap(total.astype(BF), "blk", steps[-1] | (steps[-1] >> 1 & ~1))
    return call(
        place_kernel,
        (1,),
        [whole((block, width))] * 2,
        whole((block, width)),
        S((block, width), F32),
        [],
        block * width,
        block * width * 10,
    )(l, total, got)


def solution(mesh):
    groups, layers = mesh.shape["blk"], mesh.shape["lay"]
    four = layers == 4 and groups & (groups - 1) == 0
    return jax.shard_map(
        per_device_four if four else per_device_any,
        mesh=mesh,
        in_specs=(P("blk", "lay", None), P("blk", None), P("blk", None, None), P("lay", None), P()),
        out_specs=P("lay", None),
        check_vma=False,
    )
```

```python
import jax
import jax.numpy as jnp
from jax import lax
from jax.experimental import pallas as pl
from jax.experimental.pallas import tpu as pltpu
from jax.sharding import PartitionSpec as P


TILE = 32
SUB = 16
BF = jnp.bfloat16
F32 = jnp.float32


def density_adder(left_side, dens_pattern, segment):
    count = segment.shape[0]
    block_ids = jnp.arange(count, dtype=jnp.int32) // TILE
    row_pattern = jnp.take(dens_pattern, block_ids, axis=0)
    dens_mask = jnp.repeat(row_pattern, TILE, axis=1)
    kept = jnp.where(dens_mask > 0, segment, jnp.zeros_like(segment))
    return jnp.dot(left_side, kept, preferred_element_type=jnp.float32)


def per_device_any(three_centre, metric, tile_pattern, density, dens_pattern):
    group_size = three_centre.shape[0]
    row_count = three_centre.shape[1]
    ao_width = three_centre.shape[2]
    layers = lax.axis_size("lay")
    row_start = lax.axis_index("lay") * row_count
    row_blocks = (row_start + jnp.arange(row_count, dtype=jnp.int32)) // TILE
    pattern_rows = jnp.take(tile_pattern, row_blocks, axis=1)
    tile_mask = jnp.repeat(pattern_rows, TILE, axis=2)
    masked = jnp.where(tile_mask > 0, three_centre, jnp.zeros_like(three_centre))
    coeffs = jnp.einsum("pq,qmn->pmn", metric, masked, preferred_element_type=jnp.float32).astype(
        jnp.bfloat16
    )
    left_side = coeffs.reshape(group_size * row_count, ao_width)
    inter = density_adder(
        left_side, dens_pattern, lax.all_gather(density, "lay", axis=0, tiled=True)
    )
    column_count = ao_width // layers
    inter = inter.astype(jnp.bfloat16).reshape(group_size, row_count, layers, column_count)
    outgoing = jnp.transpose(inter, (2, 1, 0, 3)).reshape(
        layers, row_count, group_size * column_count
    )
    moved = lax.all_to_all(outgoing, "lay", split_axis=0, concat_axis=1, tiled=True)
    moved = moved.reshape(ao_width, group_size * column_count)
    partial_value = jnp.dot(
        moved, coeffs.reshape(group_size * row_count, ao_width), preferred_element_type=jnp.float32
    )
    row_sums = lax.psum_scatter(partial_value, "lay", scatter_dimension=0, tiled=True)
    return lax.psum(row_sums, "blk")


def dot(a, b):
    return jnp.dot(a, b, preferred_element_type=F32)


def dot_t(a, b):
    return lax.dot_general(a, b, (((1,), (1,)), ((), ())), preferred_element_type=F32)


def iota(shape, dim):
    return lax.broadcasted_iota(jnp.int32, shape, dim)


def spread_metric(l, metric_ref, spread_ref, orders):
    group = metric_ref.shape[0]
    part = group // 4
    rows, cols = part * SUB, group * SUB
    widen = (iota((rows, part), 0) // SUB == iota((rows, part), 1)).astype(BF)
    along = (iota((group, cols), 1) // SUB == iota((group, cols), 0)).astype(BF)
    same = iota((rows, cols), 0) % SUB == iota((rows, cols), 1) % SUB
    for n, p in enumerate(orders):
        start = pl.multiple_of((l ^ p) * part, part)
        tall = dot(widen, metric_ref[pl.ds(start, part), :]).astype(BF)
        full = dot(tall, along)
        spread_ref[n * rows : (n + 1) * rows, :] = jnp.where(same, full, 0.0).astype(BF)


def masked_columns(l, order, base, three_ref, pattern_ref, first):
    group = three_ref.shape[0]
    tiles = pattern_ref.shape[1]
    block = tiles * TILE // 4
    pattern = (pattern_ref[first // TILE] > 0).astype(BF)
    out = [[] for _ in range(TILE // SUB)]
    for j in order:
        start = (l ^ j) * block
        here = (iota((tiles, block), 0) == (start // TILE) + iota((tiles, block), 1) // TILE).astype(BF)
        mask = lax.dot_general(pattern, here, (((0,), (0,)), ((), ())), preferred_element_type=F32)
        mask = jnp.broadcast_to(mask[:, None, :], (group, SUB, block)).astype(BF)
        for n, pieces in enumerate(out):
            at = first + n * SUB
            piece = three_ref[:, at : at + SUB, pl.ds(pl.multiple_of(start - base, block), block)]
            pieces.append((piece * mask).reshape(group * SUB, block))
    return [jnp.concatenate(pieces, axis=1) for pieces in out]


def near_kernel(l_ref, three_ref, metric_ref, pattern_ref, straight_ref, cross_ref, core_ref, spread_ref):
    l = l_ref[0]

    @pl.when(pl.program_id(0) == 0)
    def _():
        spread_metric(l, metric_ref, spread_ref, (2, 3))

    part, rows, width = straight_ref.shape
    block = width // 2
    for first in range(0, rows, TILE):
        strips = masked_columns(l, (0, 1), (l // 2) * width, three_ref, pattern_ref, first)
        for n, data in enumerate(strips):
            at = slice(first + n * SUB, first + (n + 1) * SUB)
            got = dot(spread_ref[...], data).astype(BF)
            straight_ref[:, at] = got[: part * SUB].reshape(part, SUB, width)
            low = got[part * SUB :].reshape(part, SUB, width)
            cross_ref[:, at] = low[:, :, :block]
            core_ref[:, at] = swapped(low, block)


def swapped(x, block):
    parts = []
    for j in range(x.shape[-1] // block):
        k = j ^ 1
        parts.append(x[..., k * block : (k + 1) * block])
    return jnp.concatenate(parts, axis=-1)


def rest_kernel(
    l_ref, three_ref, metric_ref, pattern_ref, keep_ref, send_ref, keep_far_ref, send_far_ref, spread_ref
):
    l = l_ref[0]

    @pl.when(pl.program_id(0) == 0)
    def _():
        spread_metric(l, metric_ref, spread_ref, (0, 1, 2, 3))

    part, rows, width = keep_ref.shape
    half, block = width // 2, width // 4
    one = part * SUB
    for first in range(0, rows, TILE):
        strips = masked_columns(l, (0, 1, 2, 3), 0, three_ref, pattern_ref, first)
        for n, data in enumerate(strips):
            at = slice(first + n * SUB, first + (n + 1) * SUB)
            got = dot(spread_ref[: 2 * one], data).astype(BF)
            keep_ref[:, at] = got[:one].reshape(part, SUB, width)
            send_ref[:, at] = swapped(got[one:].reshape(part, SUB, width), block)
            got = dot(spread_ref[2 * one :], data[:, half:]).astype(BF)
            keep_far_ref[:, at] = got[:one].reshape(part, SUB, half)
            send_far_ref[:, at] = swapped(got[one:].reshape(part, SUB, half), block)


def settle_kernel(l_ref, d0_ref, d1_ref, d2_ref, d3_ref, dp_ref, dens_ref, mask_ref):
    l = l_ref[0]
    block, width = d0_ref.shape
    tiles = dp_ref.shape[0]
    pat = (dp_ref[...] > 0).astype(BF)
    tall = (iota((width, tiles), 0) // TILE == iota((width, tiles), 1)).astype(BF)
    wide = (iota((tiles, width), 1) // TILE == iota((tiles, width), 0)).astype(BF)
    mask_ref[...] = dot(dot(tall, pat).astype(BF), wide)
    for i, d_ref in enumerate((d0_ref, d1_ref, d2_ref, d3_ref)):
        r = pl.multiple_of((l ^ i) * block, block)
        for j in range(4):
            c = pl.multiple_of((l ^ j) * block, block)
            tile = d_ref[:, pl.ds(c, block)].astype(F32) * mask_ref[pl.ds(r, block), pl.ds(c, block)]
            dens_ref[i * block : (i + 1) * block, j * block : (j + 1) * block] = tile.astype(BF)
            dens_ref[j * block : (j + 1) * block, width + i * block : width + (i + 1) * block] = tile.T.astype(BF)


def own_kernel(a_ref, pa_ref, b0_ref, b1_ref, pb0_ref, pb1_ref, dens_ref, inter_ref, keep_ref, send_ref, sum_ref):
    step = pl.program_id(0)
    count, block, _ = a_ref.shape
    dens = dens_ref[...]

    @pl.when(step == 0)
    def _():
        sum_ref[...] = jnp.zeros_like(sum_ref)

    total = sum_ref[...]
    for n in range(count):
        rows = jnp.concatenate([a_ref[n], pa_ref[n]], axis=0)
        inter = dot(rows, dens).astype(BF)
        inter_ref[n] = inter
        total += dot_t(inter, rows)
        top = jnp.concatenate([b0_ref[n], b1_ref[n]], axis=1)
        low = jnp.concatenate([pb0_ref[n], pb1_ref[n]], axis=1)
        rows = jnp.concatenate([top, low], axis=0)
        total += dot_t(dot(rows, dens).astype(BF), rows)
    sum_ref[...] = total

    @pl.when(step == pl.num_programs(0) - 1)
    def _():
        keep_ref[...] = total[:block]
        send_ref[...] = swapped(total[block:], block)


def local_kernel(a_ref, pa_ref, inter_ref, dens_ref, left_ref, far_ref):
    step = pl.program_id(0)
    count, _, width = a_ref.shape
    half = width // 2

    @pl.when(step == 0)
    def _():
        far_ref[...] = jnp.zeros_like(far_ref)

    dens = dens_ref[...]
    for n in range(count):
        rows = jnp.concatenate([a_ref[n], pa_ref[n]], axis=0)
        turned = dot(rows, dens).astype(BF)
        side = rows[:, half:]
        far_ref[:half] += dot(inter_ref[n, :, :half], side)
        far_ref[half:] += dot(turned[:, :half], side)
        left_ref[n, :half] = inter_ref[n, :, half:]
        left_ref[n, half:] = turned[:, half:]


def far_kernel(left_ref, straight_ref, cross_ref, begun_ref, keep_ref, send_ref, sum_ref):
    step = pl.program_id(0)
    count, block, half = straight_ref.shape

    @pl.when(step == 0)
    def _():
        sum_ref[...] = begun_ref[...]

    total = sum_ref[...]
    for n in range(count):
        top = straight_ref[n]
        low = jnp.concatenate([top[:, block:].T, cross_ref[n]], axis=1)
        total += dot(left_ref[n], jnp.concatenate([top, low], axis=0))
    sum_ref[...] = total

    @pl.when(step == pl.num_programs(0) - 1)
    def _():
        ab = total[:half]
        ba = total[half:].T
        keep_ref[:block] = ab[:block]
        keep_ref[block:] = ba[:block]
        send_ref[:block] = swapped(ab[block:], block)
        send_ref[block:] = swapped(ba[block:], block)


def place_kernel(l_ref, mine_ref, got_ref, out_ref):
    l = l_ref[0]
    block, _ = out_ref.shape
    for j in range(4):
        at = slice(j * block, (j + 1) * block)
        total = mine_ref[:, at] + got_ref[:, at].astype(F32)
        out_ref[:, pl.ds(pl.multiple_of((l ^ j) * block, block), block)] = total


def call(kernel, grid, in_specs, out_specs, out_shape, scratch, flops, nbytes, vmem=20):
    return pl.pallas_call(
        kernel,
        grid_spec=pltpu.PrefetchScalarGridSpec(
            num_scalar_prefetch=1, grid=grid, in_specs=in_specs, out_specs=out_specs, scratch_shapes=scratch
        ),
        out_shape=out_shape,
        cost_estimate=pl.CostEstimate(flops=flops, bytes_accessed=nbytes, transcendentals=0),
        compiler_params=pltpu.CompilerParams(
            dimension_semantics=("arbitrary",), vmem_limit_bytes=vmem * 1024 * 1024
        ),
    )


def no_index(kernel):
    return lambda l_ref, *refs: kernel(*refs)


def swap(x, axis, bit):
    return lax.ppermute(x, axis, [(i, i ^ bit) for i in range(lax.axis_size(axis))])


def rounded(x):
    return lax.reduce_precision(x, 8, 7)


def bits_of(groups):
    return [1 << n for n in range(groups.bit_length() - 1)]


def per_device_four(three, metric, tile_pattern, density, dens_pattern):
    return exchange_four(three, metric, tile_pattern, density, dens_pattern)


def exchange_four(three, metric, tile_pattern, density, dens_pattern):
    group, block, width = three.shape
    part, half = group // 4, width // 2
    tiles = tile_pattern.shape[2]
    index = lax.axis_index("lay")
    l = jnp.reshape(index, (1,)).astype(jnp.int32)
    S = jax.ShapeDtypeStruct
    three = pltpu.with_memory_space_constraint(three, pltpu.HBM)
    metric = pltpu.with_memory_space_constraint(metric, pltpu.HBM)
    whole = lambda shape: pl.BlockSpec(shape, lambda t, s: (0,) * len(shape))

    d2 = swap(density, "lay", 2)
    d1 = swap(density, "lay", 1)
    d3 = swap(d2, "lay", 1)

    pattern = pltpu.with_memory_space_constraint(jnp.transpose(tile_pattern, (1, 2, 0)), pltpu.HBM)
    metric_spec = pl.BlockSpec((group, group), lambda t, s: (0, 0))

    def pattern_spec(rows):
        return pl.BlockSpec((rows // TILE, tiles, group), lambda t, s: (s[0] * (block // rows) + t, 0, 0))

    rows = 2 * TILE
    strip = lambda n: pl.BlockSpec((part, 2 * TILE, n), lambda t, s: (0, t, 0))
    straight, cross, send3 = call(
        near_kernel,
        (block // rows,),
        [pl.BlockSpec((group, rows, half), lambda t, s: (0, t, s[0] // 2)), metric_spec, pattern_spec(rows)],
        [strip(half), strip(block), strip(half)],
        [S((part, block, half), BF), S((part, block, block), BF), S((part, block, half), BF)],
        [pltpu.VMEM((2 * part * SUB, group * SUB), BF)],
        4 * part * SUB * group * half * block,
        group * block * half * 4,
        vmem=24,
    )(l, three, metric, pattern)
    far_straight = swap(straight, "lay", 2)
    far_cross = swap(cross, "lay", 3)
    got3 = swap(send3, "lay", 1)

    tile = lambda n: pl.BlockSpec((part, TILE, n), lambda t, s: (0, t, 0))
    keep0, send1, keep2, send4 = call(
        rest_kernel,
        (block // TILE,),
        [pl.BlockSpec((group, TILE, width), lambda t, s: (0, t, 0)), metric_spec, pattern_spec(TILE)],
        [tile(width)] * 2 + [tile(half)] * 2,
        [S((part, block, width), BF)] * 2 + [S((part, block, half), BF)] * 2,
        [pltpu.VMEM((group * SUB, group * SUB), BF)],
        6 * part * SUB * group * width * block,
        group * block * width * 4,
        vmem=30,
    )(l, three, metric, pattern)
    got1 = swap(send1, "lay", 1)
    got4 = swap(send4, "lay", 1)

    dens = call(
        settle_kernel,
        (1,),
        [whole((block, width))] * 4 + [whole(dens_pattern.shape)],
        whole((width, 2 * width)),
        S((width, 2 * width), BF),
        [pltpu.VMEM((width, width), F32)],
        4 * width * width * tiles,
        4 * width * width * 2,
    )(l, density, d1, d2, d3, dens_pattern)

    count = 2
    many = lambda a, b: pl.BlockSpec((count, a, b), lambda t, s: (t, 0, 0))
    inter, own_keep, own_send = call(
        no_index(own_kernel),
        (part // count,),
        [many(block, width)] * 2 + [many(block, half)] * 4 + [pl.BlockSpec((width, width), lambda t, s: (0, 0))],
        [many(half, width), whole((block, half)), whole((block, half))],
        [S((part, half, width), BF), S((block, half), F32), S((block, half), F32)],
        [pltpu.VMEM((half, half), F32)],
        2 * part * 2 * half * width * (width + half),
        2 * part * half * width * 2,
    )(l, keep0, got1, straight, keep2, got3, got4, dens)
    own = own_keep + swap(own_send, "lay", 1)

    count = 4
    left, far = call(
        no_index(local_kernel),
        (part // count,),
        [many(block, width)] * 2
        + [many(half, width), pl.BlockSpec((width, width), lambda t, s: (0, 1))],
        [many(width, half), whole((width, half))],
        [S((part, width, half), BF), S((width, half), F32)],
        [],
        part * 2 * half * (width * width + 2 * half * half),
        part * half * width * 8,
    )(l, keep0, got1, inter, dens)

    count = 4
    kept, sent = call(
        no_index(far_kernel),
        (part // count,),
        [many(width, half), many(block, half), many(block, block), whole((width, half))],
        [whole((half, half))] * 2,
        [S((half, half), F32)] * 2,
        [pltpu.VMEM((width, half), F32)],
        2 * part * width * half * half,
        part * width * half * 4,
    )(l, left, far_straight, far_cross, far)
    far = kept + swap(sent, "lay", 1)
    far = far[:block] + swap(far[block:].astype(BF), "lay", 2).astype(F32)

    steps = bits_of(lax.axis_size("blk"))
    for bit in steps[:-1]:
        own = own + swap(own, "blk", bit)
        far = rounded(far)
        far = far + swap(far.astype(BF), "blk", bit).astype(F32)
    total = rounded(jnp.concatenate([own, far], axis=1))
    got = jnp.zeros(total.shape, BF)
    if steps:
        got = swap(total.astype(BF), "blk", steps[-1] | (steps[-1] >> 1 & ~1))
    return call(
        place_kernel,
        (1,),
        [whole((block, width))] * 2,
        whole((block, width)),
        S((block, width), F32),
        [],
        block * width,
        block * width * 10,
    )(l, total, got)


def solution(mesh):
    groups, layers = mesh.shape["blk"], mesh.shape["lay"]
    four = layers == 4 and groups & (groups - 1) == 0
    return jax.shard_map(
        per_device_four if four else per_device_any,
        mesh=mesh,
        in_specs=(P("blk", "lay", None), P("blk", None), P("blk", None, None), P("lay", None), P()),
        out_specs=P("lay", None),
        check_vma=False,
    )
```

```python
import jax
import jax.numpy as jnp
from jax import lax
from jax.experimental import pallas as pl
from jax.experimental.pallas import tpu as pltpu
from jax.sharding import PartitionSpec as P


TILE = 32
SUB = 16
BF = jnp.bfloat16
F32 = jnp.float32


def density_adder(left_side, dens_pattern, segment):
    count = segment.shape[0]
    block_ids = jnp.arange(count, dtype=jnp.int32) // TILE
    row_pattern = jnp.take(dens_pattern, block_ids, axis=0)
    dens_mask = jnp.repeat(row_pattern, TILE, axis=1)
    kept = jnp.where(dens_mask > 0, segment, jnp.zeros_like(segment))
    return jnp.dot(left_side, kept, preferred_element_type=jnp.float32)


def per_device_any(three_centre, metric, tile_pattern, density, dens_pattern):
    group_size = three_centre.shape[0]
    row_count = three_centre.shape[1]
    ao_width = three_centre.shape[2]
    layers = lax.axis_size("lay")
    row_start = lax.axis_index("lay") * row_count
    row_blocks = (row_start + jnp.arange(row_count, dtype=jnp.int32)) // TILE
    pattern_rows = jnp.take(tile_pattern, row_blocks, axis=1)
    tile_mask = jnp.repeat(pattern_rows, TILE, axis=2)
    masked = jnp.where(tile_mask > 0, three_centre, jnp.zeros_like(three_centre))
    coeffs = jnp.einsum("pq,qmn->pmn", metric, masked, preferred_element_type=jnp.float32).astype(
        jnp.bfloat16
    )
    left_side = coeffs.reshape(group_size * row_count, ao_width)
    inter = density_adder(
        left_side, dens_pattern, lax.all_gather(density, "lay", axis=0, tiled=True)
    )
    column_count = ao_width // layers
    inter = inter.astype(jnp.bfloat16).reshape(group_size, row_count, layers, column_count)
    outgoing = jnp.transpose(inter, (2, 1, 0, 3)).reshape(
        layers, row_count, group_size * column_count
    )
    moved = lax.all_to_all(outgoing, "lay", split_axis=0, concat_axis=1, tiled=True)
    moved = moved.reshape(ao_width, group_size * column_count)
    partial_value = jnp.dot(
        moved, coeffs.reshape(group_size * row_count, ao_width), preferred_element_type=jnp.float32
    )
    row_sums = lax.psum_scatter(partial_value, "lay", scatter_dimension=0, tiled=True)
    return lax.psum(row_sums, "blk")


def dot(a, b):
    return jnp.dot(a, b, preferred_element_type=F32)


def dot_t(a, b):
    return lax.dot_general(a, b, (((1,), (1,)), ((), ())), preferred_element_type=F32)


def iota(shape, dim):
    return lax.broadcasted_iota(jnp.int32, shape, dim)


def spread_metric(l, metric_ref, spread_ref, orders):
    group = metric_ref.shape[0]
    part = group // 4
    rows, cols = part * SUB, group * SUB
    widen = (iota((rows, part), 0) // SUB == iota((rows, part), 1)).astype(BF)
    along = (iota((group, cols), 1) // SUB == iota((group, cols), 0)).astype(BF)
    same = iota((rows, cols), 0) % SUB == iota((rows, cols), 1) % SUB
    for n, p in enumerate(orders):
        start = pl.multiple_of((l ^ p) * part, part)
        tall = dot(widen, metric_ref[pl.ds(start, part), :]).astype(BF)
        full = dot(tall, along)
        spread_ref[n * rows : (n + 1) * rows, :] = jnp.where(same, full, 0.0).astype(BF)


def masked_columns(l, order, base, three_ref, pattern_ref, first):
    group = three_ref.shape[0]
    tiles = pattern_ref.shape[1]
    block = tiles * TILE // 4
    pattern = (pattern_ref[first // TILE] > 0).astype(BF)
    out = [[] for _ in range(TILE // SUB)]
    for j in order:
        start = (l ^ j) * block
        here = (iota((tiles, block), 0) == (start // TILE) + iota((tiles, block), 1) // TILE).astype(BF)
        mask = lax.dot_general(pattern, here, (((0,), (0,)), ((), ())), preferred_element_type=F32)
        mask = jnp.broadcast_to(mask[:, None, :], (group, SUB, block)).astype(BF)
        for n, pieces in enumerate(out):
            at = first + n * SUB
            piece = three_ref[:, at : at + SUB, pl.ds(pl.multiple_of(start - base, block), block)]
            pieces.append((piece * mask).reshape(group * SUB, block))
    return [jnp.concatenate(pieces, axis=1) for pieces in out]


def near_kernel(l_ref, three_ref, metric_ref, pattern_ref, straight_ref, cross_ref, core_ref, spread_ref):
    l = l_ref[0]

    @pl.when(pl.program_id(0) == 0)
    def _():
        spread_metric(l, metric_ref, spread_ref, (2, 3))

    part, rows, width = straight_ref.shape
    block = width // 2
    for first in range(0, rows, TILE):
        strips = masked_columns(l, (0, 1), (l // 2) * width, three_ref, pattern_ref, first)
        for n, data in enumerate(strips):
            at = slice(first + n * SUB, first + (n + 1) * SUB)
            got = dot(spread_ref[...], data).astype(BF)
            straight_ref[:, at] = got[: part * SUB].reshape(part, SUB, width)
            low = got[part * SUB :].reshape(part, SUB, width)
            cross_ref[:, at] = low[:, :, :block]
            core_ref[:, at] = swapped(low, block)


def swapped(x, block):
    parts = []
    for j in range(x.shape[-1] // block):
        k = j ^ 1
        parts.append(x[..., k * block : (k + 1) * block])
    return jnp.concatenate(parts, axis=-1)


def rest_kernel(
    l_ref, three_ref, metric_ref, pattern_ref, keep_ref, send_ref, keep_far_ref, send_far_ref, spread_ref
):
    l = l_ref[0]

    @pl.when(pl.program_id(0) == 0)
    def _():
        spread_metric(l, metric_ref, spread_ref, (0, 1, 2, 3))

    part, rows, width = keep_ref.shape
    half, block = width // 2, width // 4
    one = part * SUB
    for first in range(0, rows, TILE):
        strips = masked_columns(l, (0, 1, 2, 3), 0, three_ref, pattern_ref, first)
        for n, data in enumerate(strips):
            at = slice(first + n * SUB, first + (n + 1) * SUB)
            got = dot(spread_ref[: 2 * one], data).astype(BF)
            keep_ref[:, at] = got[:one].reshape(part, SUB, width)
            send_ref[:, at] = swapped(got[one:].reshape(part, SUB, width), block)
            got = dot(spread_ref[2 * one :], data[:, half:]).astype(BF)
            keep_far_ref[:, at] = got[:one].reshape(part, SUB, half)
            send_far_ref[:, at] = swapped(got[one:].reshape(part, SUB, half), block)


def settle_kernel(l_ref, d0_ref, d1_ref, d2_ref, d3_ref, dp_ref, dens_ref, mask_ref):
    l = l_ref[0]
    block, width = d0_ref.shape
    tiles = dp_ref.shape[0]
    pat = (dp_ref[...] > 0).astype(BF)
    tall = (iota((width, tiles), 0) // TILE == iota((width, tiles), 1)).astype(BF)
    wide = (iota((tiles, width), 1) // TILE == iota((tiles, width), 0)).astype(BF)
    mask_ref[...] = dot(dot(tall, pat).astype(BF), wide)
    for i, d_ref in enumerate((d0_ref, d1_ref, d2_ref, d3_ref)):
        r = pl.multiple_of((l ^ i) * block, block)
        for j in range(4):
            c = pl.multiple_of((l ^ j) * block, block)
            tile = d_ref[:, pl.ds(c, block)].astype(F32) * mask_ref[pl.ds(r, block), pl.ds(c, block)]
            dens_ref[i * block : (i + 1) * block, j * block : (j + 1) * block] = tile.astype(BF)
            dens_ref[j * block : (j + 1) * block, width + i * block : width + (i + 1) * block] = tile.T.astype(BF)


def own_far_kernel(b0_ref, b1_ref, pb0_ref, pb1_ref, dens_ref, sum_ref):
    @pl.when(pl.program_id(0) == 0)
    def _():
        sum_ref[...] = jnp.zeros_like(sum_ref)

    dens = dens_ref[...]
    total = sum_ref[...]
    for n in range(b0_ref.shape[0]):
        top = jnp.concatenate([b0_ref[n], b1_ref[n]], axis=1)
        low = jnp.concatenate([pb0_ref[n], pb1_ref[n]], axis=1)
        rows = jnp.concatenate([top, low], axis=0)
        total += dot_t(dot(rows, dens).astype(BF), rows)
    sum_ref[...] = total


def own_kernel(a_ref, pa_ref, dens_ref, begun_ref, inter_ref, keep_ref, send_ref, sum_ref):
    step = pl.program_id(0)
    count, block, _ = a_ref.shape

    @pl.when(step == 0)
    def _():
        sum_ref[...] = begun_ref[...]

    dens = dens_ref[...]
    total = sum_ref[...]
    for n in range(count):
        rows = jnp.concatenate([a_ref[n], pa_ref[n]], axis=0)
        inter = dot(rows, dens).astype(BF)
        inter_ref[n] = inter
        total += dot_t(inter, rows)
    sum_ref[...] = total

    @pl.when(step == pl.num_programs(0) - 1)
    def _():
        keep_ref[...] = total[:block]
        send_ref[...] = swapped(total[block:], block)


def local_kernel(a_ref, pa_ref, inter_ref, dens_ref, left_ref, far_ref):
    step = pl.program_id(0)
    count, _, width = a_ref.shape
    half = width // 2

    @pl.when(step == 0)
    def _():
        far_ref[...] = jnp.zeros_like(far_ref)

    dens = dens_ref[...]
    for n in range(count):
        rows = jnp.concatenate([a_ref[n], pa_ref[n]], axis=0)
        turned = dot(rows, dens).astype(BF)
        side = rows[:, half:]
        far_ref[:half] += dot(inter_ref[n, :, :half], side)
        far_ref[half:] += dot(turned[:, :half], side)
        left_ref[n, :half] = inter_ref[n, :, half:]
        left_ref[n, half:] = turned[:, half:]


def far_kernel(left_ref, straight_ref, cross_ref, begun_ref, keep_ref, send_ref, sum_ref):
    step = pl.program_id(0)
    count, block, half = straight_ref.shape

    @pl.when(step == 0)
    def _():
        sum_ref[...] = begun_ref[...]

    total = sum_ref[...]
    for n in range(count):
        top = straight_ref[n]
        low = jnp.concatenate([top[:, block:].T, cross_ref[n]], axis=1)
        total += dot(left_ref[n], jnp.concatenate([top, low], axis=0))
    sum_ref[...] = total

    @pl.when(step == pl.num_programs(0) - 1)
    def _():
        ab = total[:half]
        ba = total[half:].T
        keep_ref[:block] = ab[:block]
        keep_ref[block:] = ba[:block]
        send_ref[:block] = swapped(ab[block:], block)
        send_ref[block:] = swapped(ba[block:], block)


def place_kernel(l_ref, mine_ref, got_ref, out_ref):
    l = l_ref[0]
    block, _ = out_ref.shape
    for j in range(4):
        at = slice(j * block, (j + 1) * block)
        total = mine_ref[:, at] + got_ref[:, at].astype(F32)
        out_ref[:, pl.ds(pl.multiple_of((l ^ j) * block, block), block)] = total


def call(kernel, grid, in_specs, out_specs, out_shape, scratch, flops, nbytes, vmem=20):
    return pl.pallas_call(
        kernel,
        grid_spec=pltpu.PrefetchScalarGridSpec(
            num_scalar_prefetch=1, grid=grid, in_specs=in_specs, out_specs=out_specs, scratch_shapes=scratch
        ),
        out_shape=out_shape,
        cost_estimate=pl.CostEstimate(flops=flops, bytes_accessed=nbytes, transcendentals=0),
        compiler_params=pltpu.CompilerParams(
            dimension_semantics=("arbitrary",), vmem_limit_bytes=vmem * 1024 * 1024
        ),
    )


def no_index(kernel):
    return lambda l_ref, *refs: kernel(*refs)


def swap(x, axis, bit):
    return lax.ppermute(x, axis, [(i, i ^ bit) for i in range(lax.axis_size(axis))])


def rounded(x):
    return lax.reduce_precision(x, 8, 7)


def bits_of(groups):
    return [1 << n for n in range(groups.bit_length() - 1)]


def per_device_four(three, metric, tile_pattern, density, dens_pattern):
    return exchange_four(three, metric, tile_pattern, density, dens_pattern)


def exchange_four(three, metric, tile_pattern, density, dens_pattern):
    group, block, width = three.shape
    part, half = group // 4, width // 2
    tiles = tile_pattern.shape[2]
    index = lax.axis_index("lay")
    l = jnp.reshape(index, (1,)).astype(jnp.int32)
    S = jax.ShapeDtypeStruct
    three = pltpu.with_memory_space_constraint(three, pltpu.HBM)
    metric = pltpu.with_memory_space_constraint(metric, pltpu.HBM)
    whole = lambda shape: pl.BlockSpec(shape, lambda t, s: (0,) * len(shape))

    d2 = swap(density, "lay", 2)
    d1 = swap(density, "lay", 1)
    d3 = swap(d2, "lay", 1)

    pattern = pltpu.with_memory_space_constraint(jnp.transpose(tile_pattern, (1, 2, 0)), pltpu.HBM)
    metric_spec = pl.BlockSpec((group, group), lambda t, s: (0, 0))

    def pattern_spec(rows):
        return pl.BlockSpec((rows // TILE, tiles, group), lambda t, s: (s[0] * (block // rows) + t, 0, 0))

    rows = 2 * TILE
    strip = lambda n: pl.BlockSpec((part, 2 * TILE, n), lambda t, s: (0, t, 0))
    straight, cross, send3 = call(
        near_kernel,
        (block // rows,),
        [pl.BlockSpec((group, rows, half), lambda t, s: (0, t, s[0] // 2)), metric_spec, pattern_spec(rows)],
        [strip(half), strip(block), strip(half)],
        [S((part, block, half), BF), S((part, block, block), BF), S((part, block, half), BF)],
        [pltpu.VMEM((2 * part * SUB, group * SUB), BF)],
        4 * part * SUB * group * half * block,
        group * block * half * 4,
        vmem=24,
    )(l, three, metric, pattern)
    far_straight = swap(straight, "lay", 2)
    far_cross = swap(cross, "lay", 3)
    got3 = swap(send3, "lay", 1)

    tile = lambda n: pl.BlockSpec((part, TILE, n), lambda t, s: (0, t, 0))
    keep0, send1, keep2, send4 = call(
        rest_kernel,
        (block // TILE,),
        [pl.BlockSpec((group, TILE, width), lambda t, s: (0, t, 0)), metric_spec, pattern_spec(TILE)],
        [tile(width)] * 2 + [tile(half)] * 2,
        [S((part, block, width), BF)] * 2 + [S((part, block, half), BF)] * 2,
        [pltpu.VMEM((group * SUB, group * SUB), BF)],
        6 * part * SUB * group * width * block,
        group * block * width * 4,
        vmem=30,
    )(l, three, metric, pattern)
    got1 = swap(send1, "lay", 1)
    got4 = swap(send4, "lay", 1)

    dens = call(
        settle_kernel,
        (1,),
        [whole((block, width))] * 4 + [whole(dens_pattern.shape)],
        whole((width, 2 * width)),
        S((width, 2 * width), BF),
        [pltpu.VMEM((width, width), F32)],
        4 * width * width * tiles,
        4 * width * width * 2,
    )(l, density, d1, d2, d3, dens_pattern)

    count = min(4, part)
    many = lambda a, b: pl.BlockSpec((count, a, b), lambda t, s: (t, 0, 0))
    square = pl.BlockSpec((width, width), lambda t, s: (0, 0))
    own_flops = 2 * part * half * width * (width + half)
    begun = call(
        no_index(own_far_kernel),
        (part // count,),
        [many(block, half)] * 4 + [square],
        whole((half, half)),
        S((half, half), F32),
        [],
        own_flops,
        part * half * width * 2,
    )(l, straight, keep2, got3, got4, dens)
    inter, own_keep, own_send = call(
        no_index(own_kernel),
        (part // count,),
        [many(block, width)] * 2 + [square, whole((half, half))],
        [many(half, width), whole((block, half)), whole((block, half))],
        [S((part, half, width), BF), S((block, half), F32), S((block, half), F32)],
        [pltpu.VMEM((half, half), F32)],
        own_flops,
        part * half * width * 4,
    )(l, keep0, got1, dens, begun)
    own = own_keep + swap(own_send, "lay", 1)

    count = min(8, part)
    left, far = call(
        no_index(local_kernel),
        (part // count,),
        [many(block, width)] * 2
        + [many(half, width), pl.BlockSpec((width, width), lambda t, s: (0, 1))],
        [many(width, half), whole((width, half))],
        [S((part, width, half), BF), S((width, half), F32)],
        [],
        part * 2 * half * (width * width + 2 * half * half),
        part * half * width * 8,
    )(l, keep0, got1, inter, dens)

    kept, sent = call(
        no_index(far_kernel),
        (part // count,),
        [many(width, half), many(block, half), many(block, block), whole((width, half))],
        [whole((half, half))] * 2,
        [S((half, half), F32)] * 2,
        [pltpu.VMEM((width, half), F32)],
        2 * part * width * half * half,
        part * width * half * 4,
    )(l, left, far_straight, far_cross, far)
    far = kept + swap(sent, "lay", 1)
    far = far[:block] + swap(far[block:].astype(BF), "lay", 2).astype(F32)

    steps = bits_of(lax.axis_size("blk"))
    for bit in steps[:-1]:
        own = own + swap(own, "blk", bit)
        far = rounded(far)
        far = far + swap(far.astype(BF), "blk", bit).astype(F32)
    total = rounded(jnp.concatenate([own, far], axis=1))
    got = jnp.zeros(total.shape, BF)
    if steps:
        got = swap(total.astype(BF), "blk", steps[-1] | (steps[-1] >> 1 & ~1))
    return call(
        place_kernel,
        (1,),
        [whole((block, width))] * 2,
        whole((block, width)),
        S((block, width), F32),
        [],
        block * width,
        block * width * 10,
    )(l, total, got)


def solution(mesh):
    groups, layers = mesh.shape["blk"], mesh.shape["lay"]
    four = layers == 4 and groups & (groups - 1) == 0
    return jax.shard_map(
        per_device_four if four else per_device_any,
        mesh=mesh,
        in_specs=(P("blk", "lay", None), P("blk", None), P("blk", None, None), P("lay", None), P()),
        out_specs=P("lay", None),
        check_vma=False,
    )
```

```python
import jax
import jax.numpy as jnp
from jax import lax
from jax.experimental import pallas as pl
from jax.experimental.pallas import tpu as pltpu
from jax.sharding import PartitionSpec as P


TILE = 32
SUB = 16
BF = jnp.bfloat16
F32 = jnp.float32


def density_adder(left_side, dens_pattern, segment):
    count = segment.shape[0]
    block_ids = jnp.arange(count, dtype=jnp.int32) // TILE
    row_pattern = jnp.take(dens_pattern, block_ids, axis=0)
    dens_mask = jnp.repeat(row_pattern, TILE, axis=1)
    kept = jnp.where(dens_mask > 0, segment, jnp.zeros_like(segment))
    return jnp.dot(left_side, kept, preferred_element_type=jnp.float32)


def per_device_any(three_centre, metric, tile_pattern, density, dens_pattern):
    group_size = three_centre.shape[0]
    row_count = three_centre.shape[1]
    ao_width = three_centre.shape[2]
    layers = lax.axis_size("lay")
    row_start = lax.axis_index("lay") * row_count
    row_blocks = (row_start + jnp.arange(row_count, dtype=jnp.int32)) // TILE
    pattern_rows = jnp.take(tile_pattern, row_blocks, axis=1)
    tile_mask = jnp.repeat(pattern_rows, TILE, axis=2)
    masked = jnp.where(tile_mask > 0, three_centre, jnp.zeros_like(three_centre))
    coeffs = jnp.einsum("pq,qmn->pmn", metric, masked, preferred_element_type=jnp.float32).astype(
        jnp.bfloat16
    )
    left_side = coeffs.reshape(group_size * row_count, ao_width)
    inter = density_adder(
        left_side, dens_pattern, lax.all_gather(density, "lay", axis=0, tiled=True)
    )
    column_count = ao_width // layers
    inter = inter.astype(jnp.bfloat16).reshape(group_size, row_count, layers, column_count)
    outgoing = jnp.transpose(inter, (2, 1, 0, 3)).reshape(
        layers, row_count, group_size * column_count
    )
    moved = lax.all_to_all(outgoing, "lay", split_axis=0, concat_axis=1, tiled=True)
    moved = moved.reshape(ao_width, group_size * column_count)
    partial_value = jnp.dot(
        moved, coeffs.reshape(group_size * row_count, ao_width), preferred_element_type=jnp.float32
    )
    row_sums = lax.psum_scatter(partial_value, "lay", scatter_dimension=0, tiled=True)
    return lax.psum(row_sums, "blk")


def dot(a, b):
    return jnp.dot(a, b, preferred_element_type=F32)


def dot_t(a, b):
    return lax.dot_general(a, b, (((1,), (1,)), ((), ())), preferred_element_type=F32)


def iota(shape, dim):
    return lax.broadcasted_iota(jnp.int32, shape, dim)


def spread_metric(l, metric_ref, spread_ref, orders):
    group = metric_ref.shape[0]
    part = group // 4
    rows, cols = part * SUB, group * SUB
    widen = (iota((rows, part), 0) // SUB == iota((rows, part), 1)).astype(BF)
    along = (iota((group, cols), 1) // SUB == iota((group, cols), 0)).astype(BF)
    same = iota((rows, cols), 0) % SUB == iota((rows, cols), 1) % SUB
    for n, p in enumerate(orders):
        start = pl.multiple_of((l ^ p) * part, part)
        tall = dot(widen, metric_ref[pl.ds(start, part), :]).astype(BF)
        full = dot(tall, along)
        spread_ref[n * rows : (n + 1) * rows, :] = jnp.where(same, full, 0.0).astype(BF)


def masked_columns(l, order, base, three_ref, pattern_ref, first):
    group = three_ref.shape[0]
    tiles = pattern_ref.shape[1]
    block = tiles * TILE // 4
    pattern = (pattern_ref[first // TILE] > 0).astype(BF)
    out = [[] for _ in range(TILE // SUB)]
    for j in order:
        start = (l ^ j) * block
        here = (iota((tiles, block), 0) == (start // TILE) + iota((tiles, block), 1) // TILE).astype(BF)
        mask = lax.dot_general(pattern, here, (((0,), (0,)), ((), ())), preferred_element_type=F32)
        mask = jnp.broadcast_to(mask[:, None, :], (group, SUB, block)).astype(BF)
        for n, pieces in enumerate(out):
            at = first + n * SUB
            piece = three_ref[:, at : at + SUB, pl.ds(pl.multiple_of(start - base, block), block)]
            pieces.append((piece * mask).reshape(group * SUB, block))
    return [jnp.concatenate(pieces, axis=1) for pieces in out]


def packed(ref, at, x, first):
    part, sub, block = x.shape
    half = block // 2
    if first < half:
        ref[:, at + first : at + first + sub] = x
        return
    corner = jnp.concatenate([x[: part // 2, :, half:], x[part // 2 :, :, half:]], axis=2)
    row = first - half
    low = row // (half // 2)
    row = at + half + row % (half // 2)
    ref[low * (part // 2) : (low + 1) * (part // 2), row : row + sub] = corner


def unpacked(ref, n, at):
    part, _, block = ref.shape
    half, quarter = block // 2, block // 4
    top = ref[n, at : at + half]
    k = n % (part // 2)
    pair = [ref[k + m * (part // 2), at + half : at + half + quarter] for m in range(2)]
    corner = jnp.concatenate(pair, axis=0)
    corner = corner[:, half:] if n >= part // 2 else corner[:, :half]
    low = jnp.concatenate([top[:, half:].T, corner], axis=1)
    return jnp.concatenate([top, low], axis=0)


def near_kernel(
    l_ref, three_ref, metric_ref, pattern_ref, straight_ref, core_ref, straight_out, cross_out, spread_ref
):
    l = l_ref[0]

    @pl.when(pl.program_id(0) == 0)
    def _():
        spread_metric(l, metric_ref, spread_ref, (2, 3))

    part, rows, width = straight_ref.shape
    block = width // 2
    steps = block // rows
    for first in range(0, rows, TILE):
        strips = masked_columns(l, (0, 1), (l // 2) * width, three_ref, pattern_ref, first)
        for n, data in enumerate(strips):
            lead = first + n * SUB
            at = slice(lead, lead + SUB)
            got = dot(spread_ref[...], data).astype(BF)
            high = got[: part * SUB].reshape(part, SUB, width)
            low = got[part * SUB :].reshape(part, SUB, width)
            straight_ref[:, at] = high
            core_ref[:, at] = swapped(low, block)
            for step in range(steps):

                @pl.when(pl.program_id(0) == step)
                def _(row=step * rows + lead):
                    straight_out[:, row : row + SUB] = high[:, :, block:]
                    packed(straight_out, block, high[:, :, :block], row)
                    packed(cross_out, 0, low[:, :, :block], row)


def swapped(x, block):
    parts = []
    for j in range(x.shape[-1] // block):
        k = j ^ 1
        parts.append(x[..., k * block : (k + 1) * block])
    return jnp.concatenate(parts, axis=-1)


def rest_kernel(
    l_ref, three_ref, metric_ref, pattern_ref, keep_ref, send_ref, keep_far_ref, send_far_ref, spread_ref
):
    l = l_ref[0]

    @pl.when(pl.program_id(0) == 0)
    def _():
        spread_metric(l, metric_ref, spread_ref, (0, 1, 2, 3))

    part, rows, width = keep_ref.shape
    half, block = width // 2, width // 4
    one = part * SUB
    for first in range(0, rows, TILE):
        strips = masked_columns(l, (0, 1, 2, 3), 0, three_ref, pattern_ref, first)
        for n, data in enumerate(strips):
            at = slice(first + n * SUB, first + (n + 1) * SUB)
            got = dot(spread_ref[: 2 * one], data).astype(BF)
            keep_ref[:, at] = got[:one].reshape(part, SUB, width)
            send_ref[:, at] = swapped(got[one:].reshape(part, SUB, width), block)
            got = dot(spread_ref[2 * one :], data[:, half:]).astype(BF)
            keep_far_ref[:, at] = got[:one].reshape(part, SUB, half)
            send_far_ref[:, at] = swapped(got[one:].reshape(part, SUB, half), block)


def settle_kernel(l_ref, d0_ref, d1_ref, d2_ref, d3_ref, dp_ref, dens_ref, mask_ref):
    l = l_ref[0]
    block, width = d0_ref.shape
    tiles = dp_ref.shape[0]
    pat = (dp_ref[...] > 0).astype(BF)
    tall = (iota((width, tiles), 0) // TILE == iota((width, tiles), 1)).astype(BF)
    wide = (iota((tiles, width), 1) // TILE == iota((tiles, width), 0)).astype(BF)
    mask_ref[...] = dot(dot(tall, pat).astype(BF), wide)
    for i, d_ref in enumerate((d0_ref, d1_ref, d2_ref, d3_ref)):
        r = pl.multiple_of((l ^ i) * block, block)
        for j in range(4):
            c = pl.multiple_of((l ^ j) * block, block)
            tile = d_ref[:, pl.ds(c, block)].astype(F32) * mask_ref[pl.ds(r, block), pl.ds(c, block)]
            dens_ref[i * block : (i + 1) * block, j * block : (j + 1) * block] = tile.astype(BF)
            dens_ref[j * block : (j + 1) * block, width + i * block : width + (i + 1) * block] = tile.T.astype(BF)


def own_far_kernel(b0_ref, b1_ref, pb0_ref, pb1_ref, dens_ref, sum_ref):
    @pl.when(pl.program_id(0) == 0)
    def _():
        sum_ref[...] = jnp.zeros_like(sum_ref)

    dens = dens_ref[...]
    total = sum_ref[...]
    for n in range(b0_ref.shape[0]):
        top = jnp.concatenate([b0_ref[n], b1_ref[n]], axis=1)
        low = jnp.concatenate([pb0_ref[n], pb1_ref[n]], axis=1)
        rows = jnp.concatenate([top, low], axis=0)
        total += dot_t(dot(rows, dens).astype(BF), rows)
    sum_ref[...] = total


def own_kernel(a_ref, pa_ref, dens_ref, begun_ref, inter_ref, keep_ref, send_ref, sum_ref):
    step = pl.program_id(0)
    count, block, _ = a_ref.shape

    @pl.when(step == 0)
    def _():
        sum_ref[...] = begun_ref[...]

    dens = dens_ref[...]
    total = sum_ref[...]
    for n in range(count):
        rows = jnp.concatenate([a_ref[n], pa_ref[n]], axis=0)
        inter = dot(rows, dens).astype(BF)
        inter_ref[n] = inter
        total += dot_t(inter, rows)
    sum_ref[...] = total

    @pl.when(step == pl.num_programs(0) - 1)
    def _():
        keep_ref[...] = total[:block]
        send_ref[...] = swapped(total[block:], block)


def local_kernel(a_ref, pa_ref, inter_ref, dens_ref, left_ref, far_ref):
    step = pl.program_id(0)
    count, _, width = a_ref.shape
    half = width // 2

    @pl.when(step == 0)
    def _():
        far_ref[...] = jnp.zeros_like(far_ref)

    dens = dens_ref[...]
    for n in range(count):
        rows = jnp.concatenate([a_ref[n], pa_ref[n]], axis=0)
        turned = dot(rows, dens).astype(BF)
        side = rows[:, half:]
        far_ref[:half] += dot(inter_ref[n, :, :half], side)
        far_ref[half:] += dot(turned[:, :half], side)
        left_ref[n, :half] = inter_ref[n, :, half:]
        left_ref[n, half:] = turned[:, half:]


def far_kernel(left_ref, straight_ref, cross_ref, begun_ref, keep_ref, send_ref):
    part, _, block = cross_ref.shape
    half = 2 * block
    total = begun_ref[...]
    for n in range(part):
        side = straight_ref[n, :block]
        top = jnp.concatenate([unpacked(straight_ref, n, block), side], axis=1)
        low = jnp.concatenate([side.T, unpacked(cross_ref, n, 0)], axis=1)
        total += dot(left_ref[n], jnp.concatenate([top, low], axis=0))
    ab = total[:half]
    ba = total[half:].T
    keep_ref[:block] = ab[:block]
    keep_ref[block:] = ba[:block]
    send_ref[:block] = swapped(ab[block:], block)
    send_ref[block:] = swapped(ba[block:], block)


def place_kernel(l_ref, mine_ref, got_ref, out_ref):
    l = l_ref[0]
    block, _ = out_ref.shape
    for j in range(4):
        at = slice(j * block, (j + 1) * block)
        total = mine_ref[:, at] + got_ref[:, at].astype(F32)
        out_ref[:, pl.ds(pl.multiple_of((l ^ j) * block, block), block)] = total


def call(kernel, grid, in_specs, out_specs, out_shape, scratch, flops, nbytes, vmem=20):
    return pl.pallas_call(
        kernel,
        grid_spec=pltpu.PrefetchScalarGridSpec(
            num_scalar_prefetch=1, grid=grid, in_specs=in_specs, out_specs=out_specs, scratch_shapes=scratch
        ),
        out_shape=out_shape,
        cost_estimate=pl.CostEstimate(flops=flops, bytes_accessed=nbytes, transcendentals=0),
        compiler_params=pltpu.CompilerParams(
            dimension_semantics=("arbitrary",), vmem_limit_bytes=vmem * 1024 * 1024
        ),
    )


def no_index(kernel):
    return lambda l_ref, *refs: kernel(*refs)


def swap(x, axis, bit):
    return lax.ppermute(x, axis, [(i, i ^ bit) for i in range(lax.axis_size(axis))])


def rounded(x):
    return lax.reduce_precision(x, 8, 7)


def bits_of(groups):
    return [1 << n for n in range(groups.bit_length() - 1)]


def per_device_four(three, metric, tile_pattern, density, dens_pattern):
    return exchange_four(three, metric, tile_pattern, density, dens_pattern)


def exchange_four(three, metric, tile_pattern, density, dens_pattern):
    group, block, width = three.shape
    part, half = group // 4, width // 2
    tiles = tile_pattern.shape[2]
    index = lax.axis_index("lay")
    l = jnp.reshape(index, (1,)).astype(jnp.int32)
    S = jax.ShapeDtypeStruct
    three = pltpu.with_memory_space_constraint(three, pltpu.HBM)
    metric = pltpu.with_memory_space_constraint(metric, pltpu.HBM)
    whole = lambda shape: pl.BlockSpec(shape, lambda t, s: (0,) * len(shape))

    d2 = swap(density, "lay", 2)
    d1 = swap(density, "lay", 1)
    d3 = swap(d2, "lay", 1)

    pattern = pltpu.with_memory_space_constraint(jnp.transpose(tile_pattern, (1, 2, 0)), pltpu.HBM)
    metric_spec = pl.BlockSpec((group, group), lambda t, s: (0, 0))

    def pattern_spec(rows):
        return pl.BlockSpec((rows // TILE, tiles, group), lambda t, s: (s[0] * (block // rows) + t, 0, 0))

    rows = block // 2
    sent = block // 2 + block // 4
    strip = lambda n: pl.BlockSpec((part, block // 2, n), lambda t, s: (0, t, 0))
    straight, send3, straight_out, cross_out = call(
        near_kernel,
        (block // rows,),
        [pl.BlockSpec((group, rows, half), lambda t, s: (0, t, s[0] // 2)), metric_spec, pattern_spec(rows)],
        [strip(half)] * 2 + [whole((part, block + sent, block)), whole((part, sent, block))],
        [S((part, block, half), BF)] * 2
        + [S((part, block + sent, block), BF), S((part, sent, block), BF)],
        [pltpu.VMEM((2 * part * SUB, group * SUB), BF)],
        4 * part * SUB * group * half * block,
        group * block * half * 4,
        vmem=24,
    )(l, three, metric, pattern)
    far_straight = swap(straight_out, "lay", 2)
    far_cross = swap(cross_out, "lay", 3)
    got3 = swap(send3, "lay", 1)

    tile = lambda n: pl.BlockSpec((part, TILE, n), lambda t, s: (0, t, 0))
    keep0, send1, keep2, send4 = call(
        rest_kernel,
        (block // TILE,),
        [pl.BlockSpec((group, TILE, width), lambda t, s: (0, t, 0)), metric_spec, pattern_spec(TILE)],
        [tile(width)] * 2 + [tile(half)] * 2,
        [S((part, block, width), BF)] * 2 + [S((part, block, half), BF)] * 2,
        [pltpu.VMEM((group * SUB, group * SUB), BF)],
        6 * part * SUB * group * width * block,
        group * block * width * 4,
        vmem=30,
    )(l, three, metric, pattern)
    got1 = swap(send1, "lay", 1)
    got4 = swap(send4, "lay", 1)

    dens = call(
        settle_kernel,
        (1,),
        [whole((block, width))] * 4 + [whole(dens_pattern.shape)],
        whole((width, 2 * width)),
        S((width, 2 * width), BF),
        [pltpu.VMEM((width, width), F32)],
        4 * width * width * tiles,
        4 * width * width * 2,
    )(l, density, d1, d2, d3, dens_pattern)

    count = min(8, part)
    many = lambda a, b: pl.BlockSpec((count, a, b), lambda t, s: (t, 0, 0))
    square = pl.BlockSpec((width, width), lambda t, s: (0, 0))
    own_flops = 2 * part * half * width * (width + half)
    begun = call(
        no_index(own_far_kernel),
        (part // count,),
        [many(block, half)] * 4 + [square],
        whole((half, half)),
        S((half, half), F32),
        [],
        own_flops,
        part * half * width * 2,
    )(l, straight, keep2, got3, got4, dens)
    inter, own_keep, own_send = call(
        no_index(own_kernel),
        (part // count,),
        [many(block, width)] * 2 + [square, whole((half, half))],
        [many(half, width), whole((block, half)), whole((block, half))],
        [S((part, half, width), BF), S((block, half), F32), S((block, half), F32)],
        [pltpu.VMEM((half, half), F32)],
        own_flops,
        part * half * width * 4,
    )(l, keep0, got1, dens, begun)
    own = own_keep + swap(own_send, "lay", 1)

    count = min(8, part)
    left, far = call(
        no_index(local_kernel),
        (part // count,),
        [many(block, width)] * 2
        + [many(half, width), pl.BlockSpec((width, width), lambda t, s: (0, 1))],
        [many(width, half), whole((width, half))],
        [S((part, width, half), BF), S((width, half), F32)],
        [],
        part * 2 * half * (width * width + 2 * half * half),
        part * half * width * 8,
    )(l, keep0, got1, inter, dens)

    kept, sent_sum = call(
        no_index(far_kernel),
        (1,),
        [
            whole((part, width, half)),
            whole((part, block + sent, block)),
            whole((part, sent, block)),
            whole((width, half)),
        ],
        [whole((half, half))] * 2,
        [S((half, half), F32)] * 2,
        [],
        2 * part * width * half * half,
        part * width * half * 4,
    )(l, left, far_straight, far_cross, far)
    far = kept + swap(sent_sum, "lay", 1)
    far = far[:block] + swap(far[block:].astype(BF), "lay", 2).astype(F32)

    steps = bits_of(lax.axis_size("blk"))
    for bit in steps[:-1]:
        own = own + swap(own, "blk", bit)
        far = rounded(far)
        far = far + swap(far.astype(BF), "blk", bit).astype(F32)
    total = rounded(jnp.concatenate([own, far], axis=1))
    got = jnp.zeros(total.shape, BF)
    if steps:
        got = swap(total.astype(BF), "blk", steps[-1] | (steps[-1] >> 1 & ~1))
    return call(
        place_kernel,
        (1,),
        [whole((block, width))] * 2,
        whole((block, width)),
        S((block, width), F32),
        [],
        block * width,
        block * width * 10,
    )(l, total, got)


def solution(mesh):
    groups, layers = mesh.shape["blk"], mesh.shape["lay"]
    four = layers == 4 and groups & (groups - 1) == 0
    return jax.shard_map(
        per_device_four if four else per_device_any,
        mesh=mesh,
        in_specs=(P("blk", "lay", None), P("blk", None), P("blk", None, None), P("lay", None), P()),
        out_specs=P("lay", None),
        check_vma=False,
    )
```

```python
import jax
import jax.numpy as jnp
from jax import lax
from jax.experimental import pallas as pl
from jax.experimental.pallas import tpu as pltpu
from jax.sharding import PartitionSpec as P


TILE = 32
SUB = 16
BF = jnp.bfloat16
F32 = jnp.float32


def density_adder(left_side, dens_pattern, segment):
    count = segment.shape[0]
    block_ids = jnp.arange(count, dtype=jnp.int32) // TILE
    row_pattern = jnp.take(dens_pattern, block_ids, axis=0)
    dens_mask = jnp.repeat(row_pattern, TILE, axis=1)
    kept = jnp.where(dens_mask > 0, segment, jnp.zeros_like(segment))
    return jnp.dot(left_side, kept, preferred_element_type=jnp.float32)


def per_device_any(three_centre, metric, tile_pattern, density, dens_pattern):
    group_size = three_centre.shape[0]
    row_count = three_centre.shape[1]
    ao_width = three_centre.shape[2]
    layers = lax.axis_size("lay")
    row_start = lax.axis_index("lay") * row_count
    row_blocks = (row_start + jnp.arange(row_count, dtype=jnp.int32)) // TILE
    pattern_rows = jnp.take(tile_pattern, row_blocks, axis=1)
    tile_mask = jnp.repeat(pattern_rows, TILE, axis=2)
    masked = jnp.where(tile_mask > 0, three_centre, jnp.zeros_like(three_centre))
    coeffs = jnp.einsum("pq,qmn->pmn", metric, masked, preferred_element_type=jnp.float32).astype(
        jnp.bfloat16
    )
    left_side = coeffs.reshape(group_size * row_count, ao_width)
    inter = density_adder(
        left_side, dens_pattern, lax.all_gather(density, "lay", axis=0, tiled=True)
    )
    column_count = ao_width // layers
    inter = inter.astype(jnp.bfloat16).reshape(group_size, row_count, layers, column_count)
    outgoing = jnp.transpose(inter, (2, 1, 0, 3)).reshape(
        layers, row_count, group_size * column_count
    )
    moved = lax.all_to_all(outgoing, "lay", split_axis=0, concat_axis=1, tiled=True)
    moved = moved.reshape(ao_width, group_size * column_count)
    partial_value = jnp.dot(
        moved, coeffs.reshape(group_size * row_count, ao_width), preferred_element_type=jnp.float32
    )
    row_sums = lax.psum_scatter(partial_value, "lay", scatter_dimension=0, tiled=True)
    return lax.psum(row_sums, "blk")


def dot(a, b):
    return jnp.dot(a, b, preferred_element_type=F32)


def dot_t(a, b):
    return lax.dot_general(a, b, (((1,), (1,)), ((), ())), preferred_element_type=F32)


def iota(shape, dim):
    return lax.broadcasted_iota(jnp.int32, shape, dim)


def spread_metric(l, metric_ref, spread_ref, orders):
    group = metric_ref.shape[0]
    part = group // 4
    rows, cols = part * SUB, group * SUB
    widen = (iota((rows, part), 0) // SUB == iota((rows, part), 1)).astype(BF)
    along = (iota((group, cols), 1) // SUB == iota((group, cols), 0)).astype(BF)
    same = iota((rows, cols), 0) % SUB == iota((rows, cols), 1) % SUB
    for n, p in enumerate(orders):
        start = pl.multiple_of((l ^ p) * part, part)
        tall = dot(widen, metric_ref[pl.ds(start, part), :]).astype(BF)
        full = dot(tall, along)
        spread_ref[n * rows : (n + 1) * rows, :] = jnp.where(same, full, 0.0).astype(BF)


def masked_columns(l, order, base, three_ref, pattern_ref, first):
    group = three_ref.shape[0]
    tiles = pattern_ref.shape[1]
    block = tiles * TILE // 4
    pattern = (pattern_ref[first // TILE] > 0).astype(BF)
    out = [[] for _ in range(TILE // SUB)]
    for j in order:
        start = (l ^ j) * block
        here = (iota((tiles, block), 0) == (start // TILE) + iota((tiles, block), 1) // TILE).astype(BF)
        mask = lax.dot_general(pattern, here, (((0,), (0,)), ((), ())), preferred_element_type=F32)
        mask = jnp.broadcast_to(mask[:, None, :], (group, SUB, block)).astype(BF)
        for n, pieces in enumerate(out):
            at = first + n * SUB
            piece = three_ref[:, at : at + SUB, pl.ds(pl.multiple_of(start - base, block), block)]
            pieces.append((piece * mask).reshape(group * SUB, block))
    return [jnp.concatenate(pieces, axis=1) for pieces in out]


def packed(ref, at, x, upper):
    part, half, _ = x.shape
    if upper:
        ref[:, at : at + half] = x
        return
    corner = jnp.concatenate([x[: part // 2, :, half:], x[part // 2 :, :, half:]], axis=2)
    row, quarter = at + half, half // 2
    ref[: part // 2, row : row + quarter] = corner[:, :quarter]
    ref[part // 2 :, row : row + quarter] = corner[:, quarter:]


def unpacked(ref, n, at):
    part, _, block = ref.shape
    half, quarter = block // 2, block // 4
    top = ref[n, at : at + half]
    k = n % (part // 2)
    pair = [ref[k + m * (part // 2), at + half : at + half + quarter] for m in range(2)]
    corner = jnp.concatenate(pair, axis=0)
    corner = corner[:, half:] if n >= part // 2 else corner[:, :half]
    low = jnp.concatenate([top[:, half:].T, corner], axis=1)
    return jnp.concatenate([top, low], axis=0)


def near_kernel(
    l_ref, three_ref, metric_ref, pattern_ref, straight_ref, core_ref, straight_out, cross_out, spread_ref
):
    l = l_ref[0]

    @pl.when(pl.program_id(0) == 0)
    def _():
        spread_metric(l, metric_ref, spread_ref, (2, 3))

    part, rows, width = straight_ref.shape
    block = width // 2
    steps = block // rows
    for first in range(0, rows, TILE):
        strips = masked_columns(l, (0, 1), (l // 2) * width, three_ref, pattern_ref, first)
        for n, data in enumerate(strips):
            lead = first + n * SUB
            at = slice(lead, lead + SUB)
            got = dot(spread_ref[...], data).astype(BF)
            high = got[: part * SUB].reshape(part, SUB, width)
            low = got[part * SUB :].reshape(part, SUB, width)
            straight_ref[:, at] = high
            core_ref[:, at] = swapped(low, block)
    straight_out[:, pl.ds(pl.multiple_of(pl.program_id(0) * rows, rows), rows)] = straight_ref[:, :, block:]
    for step in range(steps):

        @pl.when(pl.program_id(0) == step)
        def _(upper=step == 0):
            packed(straight_out, block, straight_ref[:, :, :block], upper)
            packed(cross_out, 0, core_ref[:, :, block:], upper)


def swapped(x, block):
    parts = []
    for j in range(x.shape[-1] // block):
        k = j ^ 1
        parts.append(x[..., k * block : (k + 1) * block])
    return jnp.concatenate(parts, axis=-1)


def rest_kernel(
    l_ref, three_ref, metric_ref, pattern_ref, keep_ref, send_ref, keep_far_ref, send_far_ref, spread_ref
):
    l = l_ref[0]

    @pl.when(pl.program_id(0) == 0)
    def _():
        spread_metric(l, metric_ref, spread_ref, (0, 1, 2, 3))

    part, rows, width = keep_ref.shape
    half, block = width // 2, width // 4
    one = part * SUB
    for first in range(0, rows, TILE):
        strips = masked_columns(l, (0, 1, 2, 3), 0, three_ref, pattern_ref, first)
        for n, data in enumerate(strips):
            at = slice(first + n * SUB, first + (n + 1) * SUB)
            got = dot(spread_ref[: 2 * one], data).astype(BF)
            keep_ref[:, at] = got[:one].reshape(part, SUB, width)
            send_ref[:, at] = swapped(got[one:].reshape(part, SUB, width), block)
            got = dot(spread_ref[2 * one :], data[:, half:]).astype(BF)
            keep_far_ref[:, at] = got[:one].reshape(part, SUB, half)
            send_far_ref[:, at] = swapped(got[one:].reshape(part, SUB, half), block)


def settle_kernel(l_ref, d0_ref, d1_ref, d2_ref, d3_ref, dp_ref, dens_ref, mask_ref):
    l = l_ref[0]
    block, width = d0_ref.shape
    tiles = dp_ref.shape[0]
    pat = (dp_ref[...] > 0).astype(BF)
    tall = (iota((width, tiles), 0) // TILE == iota((width, tiles), 1)).astype(BF)
    wide = (iota((tiles, width), 1) // TILE == iota((tiles, width), 0)).astype(BF)
    mask_ref[...] = dot(dot(tall, pat).astype(BF), wide)
    for i, d_ref in enumerate((d0_ref, d1_ref, d2_ref, d3_ref)):
        r = pl.multiple_of((l ^ i) * block, block)
        for j in range(4):
            c = pl.multiple_of((l ^ j) * block, block)
            tile = d_ref[:, pl.ds(c, block)].astype(F32) * mask_ref[pl.ds(r, block), pl.ds(c, block)]
            dens_ref[i * block : (i + 1) * block, j * block : (j + 1) * block] = tile.astype(BF)
            dens_ref[j * block : (j + 1) * block, width + i * block : width + (i + 1) * block] = tile.T.astype(BF)


def own_far_kernel(b0_ref, b1_ref, pb0_ref, pb1_ref, dens_ref, sum_ref):
    @pl.when(pl.program_id(0) == 0)
    def _():
        sum_ref[...] = jnp.zeros_like(sum_ref)

    dens = dens_ref[...]
    total = sum_ref[...]
    for n in range(b0_ref.shape[0]):
        top = jnp.concatenate([b0_ref[n], b1_ref[n]], axis=1)
        low = jnp.concatenate([pb0_ref[n], pb1_ref[n]], axis=1)
        rows = jnp.concatenate([top, low], axis=0)
        total += dot_t(dot(rows, dens).astype(BF), rows)
    sum_ref[...] = total


def own_kernel(a_ref, pa_ref, dens_ref, begun_ref, inter_ref, keep_ref, send_ref, sum_ref):
    step = pl.program_id(0)
    count, block, _ = a_ref.shape

    @pl.when(step == 0)
    def _():
        sum_ref[...] = begun_ref[...]

    dens = dens_ref[...]
    total = sum_ref[...]
    for n in range(count):
        rows = jnp.concatenate([a_ref[n], pa_ref[n]], axis=0)
        inter = dot(rows, dens).astype(BF)
        inter_ref[n] = inter
        total += dot_t(inter, rows)
    sum_ref[...] = total

    @pl.when(step == pl.num_programs(0) - 1)
    def _():
        keep_ref[...] = total[:block]
        send_ref[...] = swapped(total[block:], block)


def local_kernel(a_ref, pa_ref, inter_ref, dens_ref, left_ref, far_ref):
    step = pl.program_id(0)
    count, _, width = a_ref.shape
    half = width // 2

    @pl.when(step == 0)
    def _():
        far_ref[...] = jnp.zeros_like(far_ref)

    dens = dens_ref[...]
    for n in range(count):
        rows = jnp.concatenate([a_ref[n], pa_ref[n]], axis=0)
        turned = dot(rows, dens).astype(BF)
        side = rows[:, half:]
        far_ref[:half] += dot(inter_ref[n, :, :half], side)
        far_ref[half:] += dot(turned[:, :half], side)
        left_ref[n, :half] = inter_ref[n, :, half:]
        left_ref[n, half:] = turned[:, half:]


def far_kernel(left_ref, straight_ref, cross_ref, begun_ref, keep_ref, send_ref):
    part, _, block = cross_ref.shape
    half = 2 * block
    total = begun_ref[...]
    for n in range(part):
        side = straight_ref[n, :block]
        top = jnp.concatenate([unpacked(straight_ref, n, block), side], axis=1)
        low = jnp.concatenate([side.T, unpacked(cross_ref, n, 0)], axis=1)
        total += dot(left_ref[n], jnp.concatenate([top, low], axis=0))
    ab = total[:half]
    ba = total[half:].T
    keep_ref[:block] = ab[:block]
    keep_ref[block:] = ba[:block]
    send_ref[:block] = swapped(ab[block:], block)
    send_ref[block:] = swapped(ba[block:], block)


def place_kernel(l_ref, mine_ref, got_ref, out_ref):
    l = l_ref[0]
    block, _ = out_ref.shape
    for j in range(4):
        at = slice(j * block, (j + 1) * block)
        total = mine_ref[:, at] + got_ref[:, at].astype(F32)
        out_ref[:, pl.ds(pl.multiple_of((l ^ j) * block, block), block)] = total


def call(kernel, grid, in_specs, out_specs, out_shape, scratch, flops, nbytes, vmem=20):
    return pl.pallas_call(
        kernel,
        grid_spec=pltpu.PrefetchScalarGridSpec(
            num_scalar_prefetch=1, grid=grid, in_specs=in_specs, out_specs=out_specs, scratch_shapes=scratch
        ),
        out_shape=out_shape,
        cost_estimate=pl.CostEstimate(flops=flops, bytes_accessed=nbytes, transcendentals=0),
        compiler_params=pltpu.CompilerParams(
            dimension_semantics=("arbitrary",), vmem_limit_bytes=vmem * 1024 * 1024
        ),
    )


def no_index(kernel):
    return lambda l_ref, *refs: kernel(*refs)


def swap(x, axis, bit):
    return lax.ppermute(x, axis, [(i, i ^ bit) for i in range(lax.axis_size(axis))])


def rounded(x):
    return lax.reduce_precision(x, 8, 7)


def bits_of(groups):
    return [1 << n for n in range(groups.bit_length() - 1)]


def per_device_four(three, metric, tile_pattern, density, dens_pattern):
    return exchange_four(three, metric, tile_pattern, density, dens_pattern)


def exchange_four(three, metric, tile_pattern, density, dens_pattern):
    group, block, width = three.shape
    part, half = group // 4, width // 2
    tiles = tile_pattern.shape[2]
    index = lax.axis_index("lay")
    l = jnp.reshape(index, (1,)).astype(jnp.int32)
    S = jax.ShapeDtypeStruct
    three = pltpu.with_memory_space_constraint(three, pltpu.HBM)
    metric = pltpu.with_memory_space_constraint(metric, pltpu.HBM)
    whole = lambda shape: pl.BlockSpec(shape, lambda t, s: (0,) * len(shape))

    d2 = swap(density, "lay", 2)
    d1 = swap(density, "lay", 1)
    d3 = swap(d2, "lay", 1)

    pattern = pltpu.with_memory_space_constraint(jnp.transpose(tile_pattern, (1, 2, 0)), pltpu.HBM)
    metric_spec = pl.BlockSpec((group, group), lambda t, s: (0, 0))

    def pattern_spec(rows):
        return pl.BlockSpec((rows // TILE, tiles, group), lambda t, s: (s[0] * (block // rows) + t, 0, 0))

    rows = block // 2
    sent = block // 2 + block // 4
    strip = lambda n: pl.BlockSpec((part, block // 2, n), lambda t, s: (0, t, 0))
    straight, send3, straight_out, cross_out = call(
        near_kernel,
        (block // rows,),
        [pl.BlockSpec((group, rows, half), lambda t, s: (0, t, s[0] // 2)), metric_spec, pattern_spec(rows)],
        [strip(half)] * 2 + [whole((part, block + sent, block)), whole((part, sent, block))],
        [S((part, block, half), BF)] * 2
        + [S((part, block + sent, block), BF), S((part, sent, block), BF)],
        [pltpu.VMEM((2 * part * SUB, group * SUB), BF)],
        4 * part * SUB * group * half * block,
        group * block * half * 4,
        vmem=24,
    )(l, three, metric, pattern)
    far_straight = swap(straight_out, "lay", 2)
    far_cross = swap(cross_out, "lay", 3)
    got3 = swap(send3, "lay", 1)

    tile = lambda n: pl.BlockSpec((part, TILE, n), lambda t, s: (0, t, 0))
    keep0, send1, keep2, send4 = call(
        rest_kernel,
        (block // TILE,),
        [pl.BlockSpec((group, TILE, width), lambda t, s: (0, t, 0)), metric_spec, pattern_spec(TILE)],
        [tile(width)] * 2 + [tile(half)] * 2,
        [S((part, block, width), BF)] * 2 + [S((part, block, half), BF)] * 2,
        [pltpu.VMEM((group * SUB, group * SUB), BF)],
        6 * part * SUB * group * width * block,
        group * block * width * 4,
        vmem=30,
    )(l, three, metric, pattern)
    got1 = swap(send1, "lay", 1)
    got4 = swap(send4, "lay", 1)

    dens = call(
        settle_kernel,
        (1,),
        [whole((block, width))] * 4 + [whole(dens_pattern.shape)],
        whole((width, 2 * width)),
        S((width, 2 * width), BF),
        [pltpu.VMEM((width, width), F32)],
        4 * width * width * tiles,
        4 * width * width * 2,
    )(l, density, d1, d2, d3, dens_pattern)

    count = min(8, part)
    many = lambda a, b: pl.BlockSpec((count, a, b), lambda t, s: (t, 0, 0))
    square = pl.BlockSpec((width, width), lambda t, s: (0, 0))
    own_flops = 2 * part * half * width * (width + half)
    begun = call(
        no_index(own_far_kernel),
        (part // count,),
        [many(block, half)] * 4 + [square],
        whole((half, half)),
        S((half, half), F32),
        [],
        own_flops,
        part * half * width * 2,
    )(l, straight, keep2, got3, got4, dens)
    inter, own_keep, own_send = call(
        no_index(own_kernel),
        (part // count,),
        [many(block, width)] * 2 + [square, whole((half, half))],
        [many(half, width), whole((block, half)), whole((block, half))],
        [S((part, half, width), BF), S((block, half), F32), S((block, half), F32)],
        [pltpu.VMEM((half, half), F32)],
        own_flops,
        part * half * width * 4,
    )(l, keep0, got1, dens, begun)
    own = own_keep + swap(own_send, "lay", 1)

    count = min(8, part)
    left, far = call(
        no_index(local_kernel),
        (part // count,),
        [many(block, width)] * 2
        + [many(half, width), pl.BlockSpec((width, width), lambda t, s: (0, 1))],
        [many(width, half), whole((width, half))],
        [S((part, width, half), BF), S((width, half), F32)],
        [],
        part * 2 * half * (width * width + 2 * half * half),
        part * half * width * 8,
    )(l, keep0, got1, inter, dens)

    kept, sent_sum = call(
        no_index(far_kernel),
        (1,),
        [
            whole((part, width, half)),
            whole((part, block + sent, block)),
            whole((part, sent, block)),
            whole((width, half)),
        ],
        [whole((half, half))] * 2,
        [S((half, half), F32)] * 2,
        [],
        2 * part * width * half * half,
        part * width * half * 4,
    )(l, left, far_straight, far_cross, far)
    far = kept + swap(sent_sum, "lay", 1)
    far = far[:block] + swap(far[block:].astype(BF), "lay", 2).astype(F32)

    steps = bits_of(lax.axis_size("blk"))
    for bit in steps[:-1]:
        own = own + swap(own, "blk", bit)
        far = rounded(far)
        far = far + swap(far.astype(BF), "blk", bit).astype(F32)
    total = rounded(jnp.concatenate([own, far], axis=1))
    got = jnp.zeros(total.shape, BF)
    if steps:
        got = swap(total.astype(BF), "blk", steps[-1] | (steps[-1] >> 1 & ~1))
    return call(
        place_kernel,
        (1,),
        [whole((block, width))] * 2,
        whole((block, width)),
        S((block, width), F32),
        [],
        block * width,
        block * width * 10,
    )(l, total, got)


def solution(mesh):
    groups, layers = mesh.shape["blk"], mesh.shape["lay"]
    four = layers == 4 and groups & (groups - 1) == 0
    return jax.shard_map(
        per_device_four if four else per_device_any,
        mesh=mesh,
        in_specs=(P("blk", "lay", None), P("blk", None), P("blk", None, None), P("lay", None), P()),
        out_specs=P("lay", None),
        check_vma=False,
    )
```
